128 devices in a mesh: blk: 16 (over y_lo, x, core), group: 8 (over z, y_hi).
Axes of the slice: x: 4, y: 4 (y_hi: 2, y_lo: 2; y = y_hi * 2 + y_lo), z: 4, core: 2. Of those that a mesh axis runs over, the one named last changes fastest.
Arguments:
- image_embed: bfloat16 [8192, 1152], P(('blk', 'group')), may hold values from -6 to 6
- caption_vectors: bfloat16 [65536, 1152], P(('blk', 'group')), may hold values from -6 to 6
- caption_counts: int32 [8192], replicated, may hold values from 1 to 8, as said below
- natural_log_multiplier: float32 [1], replicated, may hold values from 1.5 to 2.5
- match_odds_offset: float32 [1], replicated, may hold values from -6 to -4
Outputs:
- image_grad: float32 [8192, 1152], P(('blk', 'group'))
- caption_grad: float32 [65536, 1152], P(('blk', 'group'))
The draws below stay inside these ranges and needn't reach their ends.
Inputs may be any that keep to these rules, and one draw needn't show every extreme that they name: Images are numbered as in caption_counts, 64 to a device, devices in the order of blk then group. Local image k of the device with blk index b < 8 and group index g and local image k of the device with blk index b + 8 and group index g have counts that sum to 9. On at least one device all 64 images have 8 captions.
All inputs are finite; a program needn't handle non-finite values.
Results may differ from the reference program's by a relative error of at most 0.0028.
Values may be sent and summed in bfloat16 or wider, within the bound.
No kernel may reach another device: no remote copies, remote signals or barrier semaphores. Data moves between devices by JAX's collectives and lax.ppermute only.
A program may use at most 64 MiB of HBM per device.

```python
import jax
import jax.numpy as jnp
from jax import lax

EMBED_WIDTH = 1152
NI_DEV = 64
CAP = 512
NI = 8192
CAPTION_SLOTS = 65536
N_BLK = 16
N_GROUP = 8
DEVICES = 128


def draw_caption_counts(key, part):
    half_blocks = N_BLK // 2
    level_key = jax.random.fold_in(key, 11)
    jitter_key = jax.random.fold_in(key, 12)
    flip_key = jax.random.fold_in(key, 13)
    full_key = jax.random.fold_in(key, 14)
    pair_level = jax.random.randint(level_key, (half_blocks, N_GROUP, 1), 1, 9)
    jitter = jax.random.randint(jitter_key, (half_blocks, N_GROUP, NI_DEV), -1, 2)
    lower_counts = jnp.clip(pair_level + jitter, 1, 8)
    full_pair = jax.random.randint(full_key, (), 0, half_blocks * N_GROUP)
    pair_number = jnp.arange(half_blocks * N_GROUP, dtype=jnp.int32).reshape(half_blocks, N_GROUP, 1)
    lower_counts = jnp.where(pair_number == full_pair, 8, lower_counts)
    flipped = jax.random.randint(flip_key, (half_blocks, N_GROUP, 1), 0, 2)
    lower_counts = jnp.where(flipped == 1, 9 - lower_counts, lower_counts)
    upper_counts = 9 - lower_counts
    return jnp.concatenate([lower_counts, upper_counts], axis=0).reshape(-1).astype(jnp.int32)


def centre_table(key):
    raw_centres = jax.random.normal(jax.random.fold_in(key, 21), (128, EMBED_WIDTH), jnp.float32)
    return raw_centres / jnp.sqrt(jnp.sum(raw_centres * raw_centres, axis=1, keepdims=True))


def image_clusters(key):
    return jax.random.randint(jax.random.fold_in(key, 22), (NI,), 0, 128).astype(jnp.int32)


def mixed_rows(base_key, salt, clusters, mix_low, mix_high, scale_low, scale_high):
    row_count = clusters.shape[0]
    row_key = jax.random.fold_in(base_key, salt)
    jitter_rows = jax.random.normal(jax.random.fold_in(row_key, 1), (row_count, EMBED_WIDTH), jnp.float32)
    jitter_rows = jitter_rows / jnp.sqrt(jnp.sum(jitter_rows * jitter_rows, axis=1, keepdims=True))
    mix_weight = jax.random.uniform(jax.random.fold_in(row_key, 2), (row_count, 1), jnp.float32, mix_low, mix_high)
    log_scale = jax.random.uniform(jax.random.fold_in(row_key, 3), (row_count, 1), jnp.float32, jnp.log(scale_low), jnp.log(scale_high))
    picked = jnp.take(centre_table(base_key), clusters, axis=0)
    return jnp.exp(log_scale) * (mix_weight * picked + jnp.sqrt(1.0 - mix_weight * mix_weight) * jitter_rows)


def draw_image_embed(key, part):
    clusters = image_clusters(key)
    values = mixed_rows(key, 23, clusters, 0.35, 0.85, 0.999, 1.001)
    return values.astype(jnp.bfloat16)


def draw_caption_vectors(key, part):
    counts = draw_caption_counts(key, part)
    per_device = counts.reshape(DEVICES, NI_DEV).astype(jnp.int32)
    running_end = jnp.cumsum(per_device, axis=1).astype(jnp.int32)
    position = jnp.arange(CAP, dtype=jnp.int32)
    local_index = jnp.sum((running_end[:, None, :] <= position[None, :, None]).astype(jnp.int32), axis=2).astype(jnp.int32)
    first_image = (jnp.arange(DEVICES, dtype=jnp.int32) * NI_DEV)[:, None]
    live_slots = position[None, :] < running_end[:, -1:]
    owners = jnp.where(live_slots, first_image + local_index, 0).reshape(-1).astype(jnp.int32)
    owner_clusters = jnp.take(image_clusters(key), owners)
    spare_clusters = jax.random.randint(jax.random.fold_in(key, 24), (CAPTION_SLOTS,), 0, 128).astype(jnp.int32)
    clusters = jnp.where(live_slots.reshape(-1), owner_clusters, spare_clusters).astype(jnp.int32)
    values = mixed_rows(key, 25, clusters, 0.35, 0.85, 0.999, 1.001)
    return values.astype(jnp.bfloat16)


def setup_inputs(seed: int = 0) -> dict:
    streams_of = jax.random.split(jax.random.key(seed), 6)
    image_embed = draw_image_embed(jax.random.fold_in(streams_of[5], 71), 0)
    caption_vectors = draw_caption_vectors(jax.random.fold_in(streams_of[5], 71), 0)
    caption_counts = draw_caption_counts(jax.random.fold_in(streams_of[5], 71), 0)
    natural_log_multiplier = jnp.clip(jax.random.uniform(streams_of[3], (1,), jnp.float32, 1.5, 2.5), 1.5, 2.5)
    match_odds_offset = jnp.clip(jax.random.uniform(streams_of[4], (1,), jnp.float32, -6.0, -4.0), -6.0, -4.0)
    return dict(image_embed=image_embed, caption_vectors=caption_vectors, caption_counts=caption_counts, natural_log_multiplier=natural_log_multiplier, match_odds_offset=match_odds_offset)


EPSILON = 1e-06

def normalize(embed_rows):
    values = embed_rows.astype(jnp.float32)
    inverse = lax.rsqrt(lax.optimization_barrier(jnp.sum(values * values, axis=1, keepdims=True)) + EPSILON)
    return (values * inverse, inverse)

def owner_table(caption_counts):
    per_device = caption_counts.reshape(DEVICES, NI_DEV).astype(jnp.int32)
    running_end = jnp.cumsum(per_device, axis=1).astype(jnp.int32)
    position = jnp.arange(CAP, dtype=jnp.int32)
    local_index = lax.optimization_barrier(jnp.sum((running_end[:, None, :] <= position[None, :, None]).astype(jnp.int32), axis=2)).astype(jnp.int32)
    first_image = (jnp.arange(DEVICES, dtype=jnp.int32) * NI_DEV)[:, None]
    present_entry_flags = position[None, :] < running_end[:, -1:]
    return jnp.where(present_entry_flags, first_image + local_index, -1).astype(jnp.int32)

def reference(image_embed, caption_vectors, caption_counts, natural_log_multiplier, match_odds_offset):
    image_unit, image_inverse = normalize(image_embed)
    caption_unit, caption_inverse = normalize(caption_vectors)
    image_low = image_unit.astype(jnp.bfloat16)
    caption_low = caption_unit.astype(jnp.bfloat16)
    owners = owner_table(caption_counts)
    odds_sharpness_factor = jnp.exp(natural_log_multiplier[0])
    image_ids = jnp.arange(NI, dtype=jnp.int32)
    picture_entry_extent = image_low.T

    def one_block(image_sum, inputs):
        tile_line_extent, block_owner = inputs
        similarity_matrix = odds_sharpness_factor * jnp.dot(tile_line_extent, picture_entry_extent, preferred_element_type=jnp.float32) + match_odds_offset[0]
        match_target_signs = jnp.where(block_owner[:, None] == image_ids[None, :], 1.0, -1.0)
        present_entry_flags = (block_owner >= 0)[:, None]
        oriented_similarity_gap = match_target_signs * similarity_matrix
        match_loss_factors = jnp.where(present_entry_flags, odds_sharpness_factor * (-match_target_signs * jax.nn.sigmoid(-oriented_similarity_gap)), 0.0).astype(jnp.bfloat16)
        caption_sum = jnp.dot(match_loss_factors, image_low, preferred_element_type=jnp.float32)
        image_sum = image_sum + jnp.dot(match_loss_factors.T, tile_line_extent, preferred_element_type=jnp.float32)
        return (image_sum, caption_sum)
    initial = jnp.zeros((NI, EMBED_WIDTH), jnp.float32)
    image_sum, caption_sum = lax.scan(one_block, initial, (caption_low.reshape(DEVICES, CAP, EMBED_WIDTH), owners))
    caption_sum = caption_sum.reshape(DEVICES * CAP, EMBED_WIDTH)
    image_grad = (image_sum - image_unit * lax.optimization_barrier(jnp.sum(image_unit * image_sum, axis=1, keepdims=True))) * image_inverse
    slot_live = (owners.reshape(-1) >= 0)[:, None]
    caption_grad = jnp.where(slot_live, (caption_sum - caption_unit * lax.optimization_barrier(jnp.sum(caption_unit * caption_sum, axis=1, keepdims=True))) * caption_inverse, 0.0)
    return (image_grad, caption_grad)
```

```python
import jax
import jax.numpy as jnp
from jax import lax
from jax.experimental import pallas as pl
from jax.experimental.pallas import tpu as pltpu
from jax.sharding import Mesh, PartitionSpec as P

EPSILON = 1e-06
LOG2E = 1.4426950408889634
AXES = ("y_lo", "x", "core", "z", "y_hi")
SIZES = (2, 4, 2, 4, 2)
SHIFTS = (1, 3, 2)
F32 = jnp.float32
BF16 = jnp.bfloat16
VMEM = pl.BlockSpec(memory_space=pltpu.VMEM)
SMEM = pl.BlockSpec(memory_space=pltpu.SMEM)
MIB = 2**20


def coordinates(device):
    out = []
    for size in reversed(SIZES):
        out.append(device % size)
        device //= size
    return out[::-1]


def flat(coords):
    device = 0
    for size, c in zip(SIZES, coords):
        device = device * size + c
    return device


def route(move):
    pairs = []
    for device in range(128):
        c = coordinates(device)
        move(c)
        pairs.append((device, flat(c)))
    return pairs


def ring_route(stage, distance):
    def move(c):
        axis = 1 if c[2] == stage else 3
        c[axis] = (c[axis] + distance) % 4

    return route(move)


def flip_route(axis):
    def move(c):
        c[axis] = 1 - c[axis]

    return route(move)


def send(value, pairs):
    return lax.ppermute(value, AXES, pairs)


def unit_rows(raw):
    values = raw.astype(F32)
    inverse = lax.rsqrt(jnp.sum(values * values, axis=1, keepdims=True) + EPSILON)
    return values * inverse, inverse


def merge_kernel(total_ref, own_ref, other_ref, out_ref):
    total = total_ref[0]
    rows = out_ref.shape[0]
    slots = own_ref.shape[0]
    own_low = unit_rows(own_ref[...])[0].astype(BF16)
    other_low = unit_rows(other_ref[...])[0].astype(BF16)
    position = lax.broadcasted_iota(jnp.int32, (rows, slots), 0)
    source = lax.broadcasted_iota(jnp.int32, (rows, slots), 1)
    pick_own = jnp.where((source == position) & (position < total), 1.0, 0.0).astype(BF16)
    pick_other = jnp.where(source == position - total, 1.0, 0.0).astype(BF16)
    out_ref[...] = (
        jnp.dot(pick_own, own_low, preferred_element_type=F32)
        + jnp.dot(pick_other, other_low, preferred_element_type=F32)
    ).astype(BF16)


def block_kernel(local, scalar_ref, spans_ref, images_ref, captions_ref, weight_ref, sums_ref):
    scale = scalar_ref[0]
    bias = scalar_ref[1]
    scores = lax.dot_general(
        images_ref[...], captions_ref[...], (((1,), (1,)), ((), ())), preferred_element_type=F32
    )
    steep = scores * (scale * -LOG2E) + (bias * -LOG2E)
    weight_ref[...] = (scale / (1.0 + jnp.exp2(steep))).astype(BF16)
    if local:
        count = spans_ref.shape[0]
        head = steep[:count]
        position = lax.broadcasted_iota(jnp.int32, head.shape, 1)
        match = (position >= spans_ref[:, 0:1]) & (position < spans_ref[:, 1:2])
        value = scale / (1.0 + jnp.exp2(jnp.where(match, -head, head)))
        weight_ref[:count] = jnp.where(match, -value, value).astype(BF16)
    sums_ref[...] = jnp.dot(
        weight_ref[...], captions_ref[...], preferred_element_type=F32
    ).astype(sums_ref.dtype)


def block_terms(local, scalars, spans, images, captions):
    count, width = images.shape
    slots = captions.shape[0]
    return pl.pallas_call(
        lambda *refs: block_kernel(local, *refs),
        out_shape=(
            jax.ShapeDtypeStruct((count, slots), BF16),
            jax.ShapeDtypeStruct((count, width), F32 if local else BF16),
        ),
        in_specs=[SMEM, VMEM, VMEM, VMEM],
        out_specs=(VMEM, VMEM),
        compiler_params=pltpu.CompilerParams(vmem_limit_bytes=20 * MIB),
        cost_estimate=pl.CostEstimate(
            flops=4 * count * slots * width, bytes_accessed=8 * MIB, transcendentals=count * slots
        ),
        name="block_local" if local else "block_remote",
    )(scalars, spans, images, captions)


def caption_kernel(*refs):
    own_ref, cross_ref = refs[-2:]
    half = (len(refs) - 2) // 2
    rows = own_ref.shape[0]
    total = None
    for weight_ref, images_ref in zip(refs[:half], refs[half:-2]):
        part = lax.dot_general(
            weight_ref[...], images_ref[...], (((0,), (0,)), ((), ())), preferred_element_type=F32
        )
        total = part if total is None else total + part
    own_ref[...] = total[:rows]
    cross_ref[...] = total[rows:].astype(BF16)


def caption_terms(weights, images):
    slots = weights[0].shape[1]
    width = images[0].shape[1]
    rows = sum(i.shape[0] for i in images)
    return pl.pallas_call(
        caption_kernel,
        out_shape=(
            jax.ShapeDtypeStruct((slots // 2, width), F32),
            jax.ShapeDtypeStruct((slots // 2, width), BF16),
        ),
        in_specs=[VMEM] * (2 * len(weights)),
        out_specs=(VMEM, VMEM),
        compiler_params=pltpu.CompilerParams(vmem_limit_bytes=32 * MIB),
        cost_estimate=pl.CostEstimate(
            flops=2 * rows * slots * width, bytes_accessed=8 * MIB, transcendentals=0
        ),
        name="caption_terms",
    )(*weights, *images)


def back_kernel(total_ref, own_ref, other_ref, own_out, back_out):
    total = total_ref[0]
    slots, rows = back_out.shape[0], own_ref.shape[0]
    pair = own_ref[...] + other_ref[...].astype(F32)
    own_out[...] = pair[:slots]
    target = lax.broadcasted_iota(jnp.int32, (slots, rows), 0)
    source = lax.broadcasted_iota(jnp.int32, (slots, rows), 1)
    pick = jnp.where(source == target + total, 1.0, 0.0).astype(BF16)
    back_out[...] = jnp.dot(pick, pair.astype(BF16), preferred_element_type=F32).astype(BF16)


def grad_kernel(total_ref, raw_ref, own_ref, back_ref, out_ref):
    rows = raw_ref.shape[0]
    unit, inverse = unit_rows(raw_ref[...])
    sums = own_ref[...] + back_ref[...].astype(F32)
    grads = (sums - unit * jnp.sum(unit * sums, axis=1, keepdims=True)) * inverse
    slot = pl.program_id(0) * rows + lax.broadcasted_iota(jnp.int32, grads.shape, 0)
    out_ref[...] = jnp.where(slot < total_ref[0], grads, 0.0)


def shards(image_embed, caption_vectors, caption_counts, natural_log_multiplier, match_odds_offset):
    count, width = image_embed.shape
    slots = caption_vectors.shape[0]
    pair_rows = 9 * count
    index = {a: lax.axis_index(a) for a in AXES}
    home = flat([index[a] for a in AXES])
    scale = jnp.exp(natural_log_multiplier[0])
    scalars = jnp.stack([scale, match_odds_offset[0]])

    image_unit, image_inverse = unit_rows(image_embed)
    image_low = image_unit.astype(BF16)
    far_images = send(image_low, flip_route(4))
    partner_raw = send(caption_vectors, flip_route(0))

    counts = lax.dynamic_slice_in_dim(caption_counts, home * count, count)
    earlier = lax.iota(jnp.int32, count)[None, :] <= lax.iota(jnp.int32, count)[:, None]
    ends = jnp.sum(jnp.where(earlier, counts[None, :], 0), axis=1, keepdims=True)
    spans = jnp.concatenate([ends - counts[:, None], ends], axis=1)
    total = jnp.sum(counts).reshape(1)

    near = jnp.concatenate([image_low, far_images], axis=0)
    first = [near] + [send(near, ring_route(0, k)) for k in SHIFTS]
    local_images = jnp.concatenate(first, axis=0)
    images = [local_images] + [send(local_images, ring_route(1, k)) for k in SHIFTS]

    own_pair = pl.pallas_call(
        merge_kernel,
        out_shape=jax.ShapeDtypeStruct((pair_rows, width), BF16),
        in_specs=[SMEM, VMEM, VMEM],
        out_specs=VMEM,
        compiler_params=pltpu.CompilerParams(vmem_limit_bytes=24 * MIB),
        cost_estimate=pl.CostEstimate(
            flops=4 * pair_rows * slots * width, bytes_accessed=4 * MIB, transcendentals=0
        ),
        name="merge_pair",
    )(total, caption_vectors, partner_raw)
    other_pair = send(own_pair, flip_route(2))
    captions = jnp.concatenate([own_pair, other_pair], axis=0)

    weights, partial = [], []
    for number, block in enumerate(images):
        w, p = block_terms(number == 0, scalars, spans, block, captions)
        weights.append(w)
        partial.append(p)

    image_sum = partial[0]
    for k, p in zip(SHIFTS, partial[1:]):
        image_sum = image_sum + send(p, ring_route(1, -k)).astype(F32)
    near_rows = 2 * count
    near_sum = image_sum[:near_rows]
    for number, k in enumerate(SHIFTS):
        piece = image_sum[(number + 1) * near_rows : (number + 2) * near_rows]
        near_sum = near_sum + send(piece.astype(BF16), ring_route(0, -k)).astype(F32)
    own_sum = near_sum[:count] + send(near_sum[count:].astype(BF16), flip_route(4)).astype(F32)
    image_grad = (
        own_sum - image_unit * jnp.sum(image_unit * own_sum, axis=1, keepdims=True)
    ) * image_inverse

    own_part, cross_part = caption_terms(weights, images)
    crossed = send(cross_part, flip_route(2))
    own_rows, back = pl.pallas_call(
        back_kernel,
        out_shape=(
            jax.ShapeDtypeStruct((slots, width), F32),
            jax.ShapeDtypeStruct((slots, width), BF16),
        ),
        in_specs=[SMEM, VMEM, VMEM],
        out_specs=(VMEM, VMEM),
        compiler_params=pltpu.CompilerParams(vmem_limit_bytes=24 * MIB),
        cost_estimate=pl.CostEstimate(
            flops=2 * pair_rows * slots * width, bytes_accessed=8 * MIB, transcendentals=0
        ),
        name="pair_back",
    )(total, own_part, crossed)
    returned = send(back, flip_route(0))
    tile = slots // 8
    rows_spec = pl.BlockSpec((tile, width), lambda i: (i, 0))
    caption_grad = pl.pallas_call(
        grad_kernel,
        grid=(8,),
        out_shape=jax.ShapeDtypeStruct((slots, width), F32),
        in_specs=[SMEM, rows_spec, rows_spec, rows_spec],
        out_specs=rows_spec,
        compiler_params=pltpu.CompilerParams(vmem_limit_bytes=16 * MIB),
        cost_estimate=pl.CostEstimate(
            flops=16 * slots * width, bytes_accessed=8 * MIB, transcendentals=0
        ),
        name="caption_grad",
    )(total, caption_vectors, own_rows, returned)
    return image_grad, caption_grad


def solution(mesh):
    fine = Mesh(mesh.devices.reshape(SIZES), AXES)
    placed = (P(AXES, None), P(AXES, None), P(), P(), P())
    return jax.shard_map(
        shards,
        mesh=fine,
        in_specs=placed,
        out_specs=(P(AXES, None), P(AXES, None)),
        check_vma=False,
    )
```

```python
import functools

import jax
import jax.numpy as jnp
from jax import lax
from jax.experimental import pallas as pl
from jax.experimental.pallas import tpu as pltpu
from jax.sharding import Mesh, PartitionSpec as P


EPSILON = 1e-06
LOG2E = 1.4426950408889634
AXES = ("y_lo", "x", "core", "z", "y_hi")
SIZES = (2, 4, 2, 4, 2)
F32 = jnp.float32
BF16 = jnp.bfloat16
VMEM = pl.BlockSpec(memory_space=pltpu.VMEM)
ANY = pl.BlockSpec(memory_space=pl.ANY)
SMEM = pl.BlockSpec(memory_space=pltpu.SMEM)
MIB = 2**20


def coordinates(device):
    out = []
    for size in reversed(SIZES):
        out.append(device % size)
        device //= size
    return out[::-1]


def flat(coords):
    device = 0
    for size, c in zip(SIZES, coords):
        device = device * size + c
    return device


def route(move):
    pairs = []
    for device in range(128):
        c = coordinates(device)
        move(c)
        pairs.append((device, flat(c)))
    return pairs


def ring_route(stage, distance):
    def move(c):
        axis = 1 if c[2] == stage else 3
        c[axis] = (c[axis] + distance) % 4

    return route(move)


def flip_route(axis):
    def move(c):
        c[axis] = 1 - c[axis]

    return route(move)


def send(value, pairs):
    return lax.ppermute(value, AXES, pairs)


def unit_rows(raw):
    values = raw.astype(F32)
    inverse = lax.rsqrt(jnp.sum(values * values, axis=1, keepdims=True) + EPSILON)
    return values * inverse, inverse


def near_kernel(own_ref, far_ref, near_ref):
    count = own_ref.shape[0]
    near_ref[:count] = unit_rows(own_ref[...])[0].astype(BF16)
    near_ref[count:] = unit_rows(far_ref[...])[0].astype(BF16)


def join_kernel(*refs):
    rows = refs[0].shape[0]
    refs[-2][:rows] = refs[0][...]
    refs[-2][rows:] = refs[1][...]
    refs[-1][:rows] = refs[2][...]
    refs[-1][rows:] = refs[3][...]


def plain(kernel, out_shape, args, flops=10**6, smem=0, limit=16, after=()):
    return pl.pallas_call(
        lambda *refs: kernel(*refs[: len(args)], *refs[len(args) + len(after) :]),
        out_shape=out_shape,
        in_specs=[SMEM] * smem + [VMEM] * (len(args) - smem) + [ANY] * len(after),
        out_specs=(VMEM,) * len(out_shape) if isinstance(out_shape, tuple) else VMEM,
        compiler_params=pltpu.CompilerParams(vmem_limit_bytes=limit * MIB),
        cost_estimate=pl.CostEstimate(flops=flops, bytes_accessed=MIB, transcendentals=0),
    )(*args, *after)


def prep_kernel(total_ref, own_ref, early_ref, late_ref):
    slots = own_ref.shape[0]
    early = early_ref.shape[0]
    low = unit_rows(own_ref[...])[0]
    slot = lax.broadcasted_iota(jnp.int32, low.shape, 0)
    low = jnp.where(slot < total_ref[0], low, 0.0).astype(BF16)
    early_ref[...] = low[:early]
    late_ref[: slots - early] = low[early:]
    late_ref[slots - early :] = jnp.zeros((late_ref.shape[0] - slots + early, low.shape[1]), BF16)


def picked(rows, columns, offset, values):
    row = lax.broadcasted_iota(jnp.int32, (rows, columns), 0)
    column = lax.broadcasted_iota(jnp.int32, (rows, columns), 1)
    pick = jnp.where(column == row + offset, 1.0, 0.0).astype(BF16)
    return jnp.dot(pick, values, preferred_element_type=F32)


def merge_kernel(start, parts, total_ref, own_ref, *refs):
    out_ref = refs[-1]
    rows = out_ref.shape[0]
    merged = own_ref[...].astype(F32)
    for number in range(parts):
        raw = refs[number][...]
        low = unit_rows(raw)[0].astype(BF16)
        offset = start - number * raw.shape[0] - total_ref[0]
        merged = merged + picked(rows, raw.shape[0], offset, low)
    out_ref[...] = merged.astype(BF16)


def stack(own_ref, other_ref, out_ref):
    rows = own_ref.shape[0]
    out_ref[:256] = own_ref[:256]
    out_ref[256:512] = other_ref[:256]
    if rows > 256:
        out_ref[512 : rows + 256] = own_ref[256:]
        out_ref[rows + 256 :] = other_ref[256:]


def weigh(local, start, scalar_ref, spans_ref, images, captions, weight_ref):
    scale = scalar_ref[0]
    bias = scalar_ref[1]
    scores = lax.dot_general(
        images, captions, (((1,), (1,)), ((), ())), preferred_element_type=F32
    )
    steep = scores * (scale * -LOG2E) + (bias * -LOG2E)
    weight_ref[...] = (scale / (1.0 + jnp.exp2(steep))).astype(BF16)
    if local:
        count = spans_ref.shape[0]
        head = steep[:count]
        column = lax.broadcasted_iota(jnp.int32, head.shape, 1)
        rest = (column >= 512) & (column < 576)
        position = jnp.where(column < 256, column, jnp.where(rest, column - 256, -1 - start)) + start
        match = (position >= spans_ref[:, 0:1]) & (position < spans_ref[:, 1:2])
        value = scale / (1.0 + jnp.exp2(jnp.where(match, -head, head)))
        weight_ref[:count] = jnp.where(match, -value, value).astype(BF16)


def early_kernel(
    local, scalar_ref, spans_ref, head_ref, tail_ref, own_ref, other_ref, *refs
):
    weight_ref, images_ref, sums_ref, captions_ref = refs[-4:]
    rows = head_ref.shape[0]
    images_ref[:rows] = head_ref[...]
    images_ref[rows:] = tail_ref[...]
    stack(own_ref, other_ref, captions_ref)
    weigh(local, 0, scalar_ref, spans_ref, images_ref[...], captions_ref[...], weight_ref)
    sums_ref[...] = jnp.dot(weight_ref[...], captions_ref[...], preferred_element_type=F32)


def late_kernel(
    local, start, scalar_ref, spans_ref, images_ref, sums_ref, own_ref, other_ref, *refs
):
    weight_ref, head_out, tail_out, captions_ref = refs[-4:]
    rows = head_out.shape[0]
    stack(own_ref, other_ref, captions_ref)
    weigh(local, start, scalar_ref, spans_ref, images_ref[...], captions_ref[...], weight_ref)
    sums = sums_ref[...] + jnp.dot(
        weight_ref[...], captions_ref[...], preferred_element_type=F32
    )
    head_out[...] = sums[:rows].astype(head_out.dtype)
    tail_out[...] = sums[rows:].astype(tail_out.dtype)


def early_terms(local, scalars, spans, head, tail, own, other, after=()):
    rows, width = head.shape
    slots = 2 * own.shape[0]
    return pl.pallas_call(
        lambda *refs: early_kernel(local, *refs),
        out_shape=(
            jax.ShapeDtypeStruct((2 * rows, slots), BF16),
            jax.ShapeDtypeStruct((2 * rows, width), BF16),
            jax.ShapeDtypeStruct((2 * rows, width), F32),
        ),
        in_specs=[SMEM, VMEM, VMEM, VMEM, VMEM, VMEM] + [ANY] * len(after),
        out_specs=(VMEM,) * 3,
        scratch_shapes=[pltpu.VMEM((slots, width), BF16)],
        compiler_params=pltpu.CompilerParams(vmem_limit_bytes=20 * MIB),
        cost_estimate=pl.CostEstimate(
            flops=8 * rows * slots * width, bytes_accessed=8 * MIB, transcendentals=2 * rows * slots
        ),
        name="early_local" if local else "early_remote",
    )(scalars, spans, head, tail, own, other, *after)


def late_terms(local, start, scalars, spans, images, sums, own, other, types, after=()):
    rows, width = images.shape
    slots = 2 * own.shape[0]
    return pl.pallas_call(
        lambda *refs: late_kernel(local, start, *refs),
        out_shape=(
            jax.ShapeDtypeStruct((rows, slots), BF16),
            jax.ShapeDtypeStruct((rows // 2, width), types[0]),
            jax.ShapeDtypeStruct((rows // 2, width), types[1]),
        ),
        in_specs=[SMEM, VMEM, VMEM, VMEM, VMEM, VMEM] + [ANY] * len(after),
        out_specs=(VMEM,) * 3,
        scratch_shapes=[pltpu.VMEM((slots, width), BF16)],
        compiler_params=pltpu.CompilerParams(vmem_limit_bytes=20 * MIB),
        cost_estimate=pl.CostEstimate(
            flops=4 * rows * slots * width, bytes_accessed=8 * MIB, transcendentals=rows * slots
        ),
        name="late_local" if local else "late_remote",
    )(scalars, spans, images, sums, own, other, *after)


def caption_kernel(blocks, *refs):
    own_ref, cross_ref = refs[-2:]
    rows = own_ref.shape[0]
    total = None
    for weight_ref, images_ref in zip(refs[:blocks], refs[blocks : 2 * blocks]):
        part = lax.dot_general(
            weight_ref[...], images_ref[...], (((0,), (0,)), ((), ())), preferred_element_type=F32
        )
        total = part if total is None else total + part
    own_ref[:256] = total[:256]
    cross_ref[:256] = total[256:512].astype(BF16)
    if rows > 256:
        own_ref[256:] = total[512 : rows + 256]
        cross_ref[256:] = total[rows + 256 :].astype(BF16)


def caption_terms(weights, images, after=()):
    slots = weights[0].shape[1]
    width = images[0].shape[1]
    rows = sum(i.shape[0] for i in images)
    return pl.pallas_call(
        lambda *refs: caption_kernel(len(weights), *refs),
        out_shape=(
            jax.ShapeDtypeStruct((slots // 2, width), F32),
            jax.ShapeDtypeStruct((slots // 2, width), BF16),
        ),
        in_specs=[VMEM] * (2 * len(weights)) + [ANY] * len(after),
        out_specs=(VMEM, VMEM),
        compiler_params=pltpu.CompilerParams(vmem_limit_bytes=24 * MIB),
        cost_estimate=pl.CostEstimate(
            flops=2 * rows * slots * width, bytes_accessed=8 * MIB, transcendentals=0
        ),
        name="caption_terms",
    )(*weights, *images, *after)


def pair_kernel(skip, own_ref, cross_ref, pair_ref, back_ref):
    pair = own_ref[...] + cross_ref[...].astype(F32)
    pair_ref[...] = pair
    back_ref[...] = pair[skip:].astype(BF16)


def home_kernel(total_ref, early_ref, late_ref, back_ref, out_ref):
    slots = out_ref.shape[0]
    early = early_ref.shape[0]
    back = picked(slots, back_ref.shape[0], slots // 2 - total_ref[0], back_ref[...])
    out_ref[:early] = back[:early] + early_ref[...]
    out_ref[early:] = back[early:] + late_ref[: slots - early]


def grad_kernel(total_ref, raw_ref, own_ref, back_ref, out_ref):
    rows = out_ref.shape[0]
    start = pl.program_id(0) * rows
    unit, inverse = unit_rows(raw_ref[...])
    offset = start + pl.num_programs(0) * rows - total_ref[0]
    sums = own_ref[...] + picked(rows, back_ref.shape[0], offset, back_ref[...])
    grads = (sums - unit * jnp.sum(unit * sums, axis=1, keepdims=True)) * inverse
    slot = start + lax.broadcasted_iota(jnp.int32, grads.shape, 0)
    out_ref[...] = jnp.where(slot < total_ref[0], grads, 0.0)


def caption_grads(total, raw, own_rows, back):
    slots, width = raw.shape
    steps = 4
    some = pl.BlockSpec((slots // steps, width), lambda i: (i, 0))
    return pl.pallas_call(
        grad_kernel,
        grid=(steps,),
        out_shape=jax.ShapeDtypeStruct((slots, width), F32),
        in_specs=[SMEM, some, some, pl.BlockSpec(back.shape, lambda i: (0, 0))],
        out_specs=some,
        compiler_params=pltpu.CompilerParams(vmem_limit_bytes=16 * MIB),
        cost_estimate=pl.CostEstimate(
            flops=8 * slots * width, bytes_accessed=4 * MIB, transcendentals=0
        ),
        name="caption_grad",
    )(total, raw, own_rows, back)


def program(image_embed, caption_vectors, caption_counts, natural_log_multiplier, match_odds_offset):
    count, width = image_embed.shape
    slots = caption_vectors.shape[0]
    pair_rows = 9 * count
    index = {a: lax.axis_index(a) for a in AXES}
    home = flat([index[a] for a in AXES])
    scale = jnp.exp(natural_log_multiplier[0])
    scalars = jnp.stack([scale, match_odds_offset[0]])

    far_raw = send(image_embed, flip_route(4))
    half_slots = slots // 2
    partner_a = send(caption_vectors[:half_slots], flip_route(0))
    partner_b = send(caption_vectors[half_slots:], flip_route(0))

    counts = lax.dynamic_slice_in_dim(caption_counts, home * count, count)
    earlier = lax.iota(jnp.int32, count)[None, :] <= lax.iota(jnp.int32, count)[:, None]
    ends = jnp.sum(jnp.where(earlier, counts[None, :], 0), axis=1, keepdims=True)
    spans = jnp.concatenate([ends - counts[:, None], ends], axis=1)
    total = jnp.sum(counts).reshape(1)

    half = jax.ShapeDtypeStruct((4 * count, width), BF16)
    near = plain(
        near_kernel, jax.ShapeDtypeStruct((2 * count, width), BF16), (image_embed, far_raw)
    )
    first = {}
    for k in (2, 1, 3):
        first[k] = send(near, ring_route(0, k))
    head, tail = plain(join_kernel, (half, half), (near, first[1], first[3], first[2]))
    up_head = send(head, ring_route(1, 1))
    down_tail = send(tail, ring_route(1, 3))
    up_tail = send(tail, ring_route(1, 1))
    down_head = send(head, ring_route(1, 3))
    two_head = send(up_head, ring_route(1, 1))
    two_tail = send(down_tail, ring_route(1, 3))

    late_rows = half_slots
    early_rows = pair_rows - late_rows
    early_shape = jax.ShapeDtypeStruct((early_rows, width), BF16)
    late_shape = jax.ShapeDtypeStruct((late_rows, width), BF16)
    own_early, own_late = plain(
        prep_kernel, (early_shape, late_shape), (total, caption_vectors), smem=1
    )
    merge_flops = 2 * early_rows * half_slots * width
    early_own = plain(
        functools.partial(merge_kernel, 0, 1),
        early_shape,
        (total, own_early, partner_a),
        merge_flops,
        1,
        after=(head,),
    )
    early_other = send(early_own, flip_route(2))
    late_own = plain(
        functools.partial(merge_kernel, early_rows, 2),
        late_shape,
        (total, own_late, partner_a, partner_b),
        2 * merge_flops,
        1,
        after=(up_head, down_tail),
    )
    late_other = send(late_own, flip_route(2))

    def early(head, tail, local=False, after=()):
        return early_terms(local, scalars, spans, head, tail, early_own, early_other, after)

    def late(images, sums, types, local=False, after=()):
        return late_terms(
            local, early_rows, scalars, spans, images, sums, late_own, late_other, types, after
        )

    we_local, i_local, s_local = early(head, tail, True)
    we_up, i_up, s_up = early(up_head, up_tail)
    we_down, i_down, s_down = early(down_head, down_tail)
    wl_up, up_a, up_b = late(i_up, s_up, (BF16, F32), after=(we_down,))
    from_above = send(up_a, ring_route(1, 3)).astype(F32)
    wl_down, down_a, down_b = late(i_down, s_down, (F32, BF16))
    from_below = send(down_b, ring_route(1, 1)).astype(F32)
    we_two, i_two, s_two = early(two_head, two_tail, after=(wl_up, wl_down))
    wl_two, two_a, two_b = late(i_two, s_two, (BF16, BF16))
    over_head = send(two_a, ring_route(1, 1)).astype(F32)
    over_tail = send(two_b, ring_route(1, 3)).astype(F32)
    wl_local, local_a, local_b = late(i_local, s_local, (F32, F32), True, after=(wl_two,))
    images = [i_up, i_down, i_two, i_local]
    late_part, late_cross = caption_terms([wl_up, wl_down, wl_two, wl_local], images)
    late_crossed = send(late_cross, flip_route(2))
    early_part, early_cross = caption_terms(
        [we_up, we_down, we_two, we_local], images, after=(late_part,)
    )
    early_crossed = send(early_cross, flip_route(2))
    head_below = send((down_a + over_head).astype(BF16), ring_route(1, 1)).astype(F32)
    tail_above = send((up_b + over_tail).astype(BF16), ring_route(1, 3)).astype(F32)
    back_shape = jax.ShapeDtypeStruct((half_slots, width), BF16)
    late_pair, late_back = plain(
        functools.partial(pair_kernel, 0),
        (jax.ShapeDtypeStruct((late_rows, width), F32), back_shape),
        (late_part, late_crossed),
    )
    returned_late = send(late_back, flip_route(0))
    early_pair, early_back = plain(
        functools.partial(pair_kernel, early_rows - half_slots),
        (jax.ShapeDtypeStruct((early_rows, width), F32), back_shape),
        (early_part, early_crossed),
    )
    returned_early = send(early_back, flip_route(0))
    head_sum = local_a + from_above + head_below
    tail_sum = local_b + from_below + tail_above

    near_rows = 2 * count
    pieces = {1: head_sum[near_rows:], 3: tail_sum[:near_rows], 2: tail_sum[near_rows:]}
    near_sum = head_sum[:near_rows]
    for k in (2, 1, 3):
        near_sum = near_sum + send(pieces[k].astype(BF16), ring_route(0, -k)).astype(F32)
    far_sum = send(near_sum[count:].astype(BF16), flip_route(4)).astype(F32)
    own_sum = near_sum[:count] + far_sum
    image_unit, image_inverse = unit_rows(image_embed)
    image_grad = (
        own_sum - image_unit * jnp.sum(image_unit * own_sum, axis=1, keepdims=True)
    ) * image_inverse

    own_rows = plain(
        home_kernel,
        jax.ShapeDtypeStruct((slots, width), F32),
        (total, early_pair, late_pair, returned_late),
        2 * slots * half_slots * width,
        1,
    )
    caption_grad = caption_grads(total, caption_vectors, own_rows, returned_early)
    return image_grad, caption_grad


def solution(mesh):
    fine = Mesh(mesh.devices.reshape(SIZES), AXES)
    placed = (P(AXES, None), P(AXES, None), P(), P(), P())
    return jax.shard_map(
        program,
        mesh=fine,
        in_specs=placed,
        out_specs=(P(AXES, None), P(AXES, None)),
        check_vma=False,
    )
```

```python
import functools

import jax
import jax.numpy as jnp
from jax import lax
from jax.experimental import pallas as pl
from jax.experimental.pallas import tpu as pltpu
from jax.sharding import Mesh, PartitionSpec as P


EPSILON = 1e-06
LOG2E = 1.4426950408889634
AXES = ("y_lo", "x", "core", "z", "y_hi")
SIZES = (2, 4, 2, 4, 2)
F32 = jnp.float32
BF16 = jnp.bfloat16
VMEM = pl.BlockSpec(memory_space=pltpu.VMEM)
ANY = pl.BlockSpec(memory_space=pl.ANY)
SMEM = pl.BlockSpec(memory_space=pltpu.SMEM)
MIB = 2**20


def coordinates(device):
    out = []
    for size in reversed(SIZES):
        out.append(device % size)
        device //= size
    return out[::-1]


def flat(coords):
    device = 0
    for size, c in zip(SIZES, coords):
        device = device * size + c
    return device


def route(move):
    pairs = []
    for device in range(128):
        c = coordinates(device)
        move(c)
        pairs.append((device, flat(c)))
    return pairs


def ring_route(stage, distance):
    def move(c):
        axis = 1 if c[2] == stage else 3
        c[axis] = (c[axis] + distance) % 4

    return route(move)


def flip_route(axis):
    def move(c):
        c[axis] = 1 - c[axis]

    return route(move)


def send(value, pairs):
    return lax.ppermute(value, AXES, pairs)


def unit_rows(raw):
    values = raw.astype(F32)
    inverse = lax.rsqrt(jnp.sum(values * values, axis=1, keepdims=True) + EPSILON)
    return values * inverse, inverse


def near_kernel(own_ref, far_ref, near_ref):
    count = own_ref.shape[0]
    near_ref[:count] = unit_rows(own_ref[...])[0].astype(BF16)
    near_ref[count:] = unit_rows(far_ref[...])[0].astype(BF16)


def join_kernel(*refs):
    rows = refs[0].shape[0]
    refs[-2][:rows] = refs[0][...]
    refs[-2][rows:] = refs[1][...]
    refs[-1][:rows] = refs[2][...]
    refs[-1][rows:] = refs[3][...]


def plain(kernel, out_shape, args, flops=10**6, smem=0, limit=16, after=()):
    return pl.pallas_call(
        lambda *refs: kernel(*refs[: len(args)], *refs[len(args) + len(after) :]),
        out_shape=out_shape,
        in_specs=[SMEM] * smem + [VMEM] * (len(args) - smem) + [ANY] * len(after),
        out_specs=(VMEM,) * len(out_shape) if isinstance(out_shape, tuple) else VMEM,
        compiler_params=pltpu.CompilerParams(vmem_limit_bytes=limit * MIB),
        cost_estimate=pl.CostEstimate(flops=flops, bytes_accessed=MIB, transcendentals=0),
    )(*args, *after)


def prep_kernel(total_ref, own_ref, out_ref):
    slots = own_ref.shape[0]
    low = unit_rows(own_ref[...])[0]
    slot = lax.broadcasted_iota(jnp.int32, low.shape, 0)
    out_ref[:slots] = jnp.where(slot < total_ref[0], low, 0.0).astype(BF16)
    out_ref[slots:] = jnp.zeros((out_ref.shape[0] - slots, low.shape[1]), BF16)


def picked(rows, columns, offset, values):
    row = lax.broadcasted_iota(jnp.int32, (rows, columns), 0)
    column = lax.broadcasted_iota(jnp.int32, (rows, columns), 1)
    pick = jnp.where(column == row + offset, 1.0, 0.0).astype(BF16)
    return jnp.dot(pick, values, preferred_element_type=F32)


def merge_kernel(total_ref, own_ref, raw_ref, out_ref):
    low = unit_rows(raw_ref[...])[0].astype(BF16)
    other = picked(out_ref.shape[0], low.shape[0], -total_ref[0], low)
    out_ref[...] = (own_ref[...].astype(F32) + other).astype(BF16)


def stack_kernel(own_ref, other_ref, out_ref):
    rows = own_ref.shape[0]
    out_ref[:512] = own_ref[:512]
    out_ref[512:1024] = other_ref[:512]
    out_ref[1024 : rows + 512] = own_ref[512:]
    out_ref[rows + 512 :] = other_ref[512:]


def weigh(local, scalar_ref, spans_ref, images, captions, weight_ref):
    scale = scalar_ref[0]
    bias = scalar_ref[1]
    scores = lax.dot_general(
        images, captions, (((1,), (1,)), ((), ())), preferred_element_type=F32
    )
    steep = scores * (scale * -LOG2E) + (bias * -LOG2E)
    weight_ref[...] = (scale / (1.0 + jnp.exp2(steep))).astype(BF16)
    if local:
        count = spans_ref.shape[0]
        head = steep[:count, :512]
        slot = lax.broadcasted_iota(jnp.int32, head.shape, 1)
        match = (slot >= spans_ref[:, 0:1]) & (slot < spans_ref[:, 1:2])
        value = scale / (1.0 + jnp.exp2(jnp.where(match, -head, head)))
        weight_ref[:count, :512] = jnp.where(match, -value, value).astype(BF16)


def weight_kernel(
    local, sums, scalar_ref, spans_ref, head_ref, tail_ref, captions_ref, weight_ref, images_ref,
    *outs,
):
    rows = head_ref.shape[0]
    images_ref[:rows] = head_ref[...]
    images_ref[rows:] = tail_ref[...]
    weigh(local, scalar_ref, spans_ref, images_ref[...], captions_ref[...], weight_ref)
    if sums:
        total = jnp.dot(weight_ref[...], captions_ref[...], preferred_element_type=F32)
        outs[0][...] = total[:rows].astype(outs[0].dtype)
        outs[1][...] = total[rows:].astype(outs[1].dtype)


def weight_terms(local, types, scalars, spans, head, tail, captions, after=()):
    rows, width = head.shape
    slots = captions.shape[0]
    arity = 5
    return pl.pallas_call(
        lambda *refs: weight_kernel(
            local, bool(types), *refs[:arity], *refs[arity + len(after) :]
        ),
        out_shape=(
            jax.ShapeDtypeStruct((2 * rows, slots), BF16),
            jax.ShapeDtypeStruct((2 * rows, width), BF16),
            *[jax.ShapeDtypeStruct((rows, width), t) for t in types],
        ),
        in_specs=[SMEM] + [VMEM] * (arity - 1) + [ANY] * len(after),
        out_specs=(VMEM,) * (2 + len(types)),
        compiler_params=pltpu.CompilerParams(vmem_limit_bytes=20 * MIB),
        cost_estimate=pl.CostEstimate(
            flops=(8 if types else 4) * rows * slots * width,
            bytes_accessed=8 * MIB,
            transcendentals=2 * rows * slots,
        ),
        name="block_local" if local else "block_remote",
    )(scalars, spans, head, tail, captions, *after)


def local_sums_kernel(weight_ref, captions_ref, head_out, tail_out):
    rows = head_out.shape[0]
    total = jnp.dot(weight_ref[...], captions_ref[...], preferred_element_type=F32)
    head_out[...] = total[:rows]
    tail_out[...] = total[rows:]


def caption_sum(refs, blocks, columns):
    total = None
    for weight_ref, images_ref in zip(refs[:blocks], refs[blocks : 2 * blocks]):
        part = lax.dot_general(
            weight_ref[:, columns], images_ref[...], (((0,), (0,)), ((), ())),
            preferred_element_type=F32,
        )
        total = part if total is None else total + part
    return total


def cross_kernel(blocks, *refs):
    cross_ref, tail_ref = refs[-2:]
    rest = tail_ref.shape[0]
    total = caption_sum(refs, blocks, slice(512, refs[0].shape[1]))
    cross_ref[:512] = total[:512].astype(BF16)
    tail_ref[...] = total[512 : 512 + rest]
    cross_ref[512:] = total[512 + rest :].astype(BF16)


def own_kernel(blocks, *refs):
    refs[-1][...] = caption_sum(refs, blocks, slice(0, 512))


def combine_kernel(down_a, down_b, over_head, up_a, up_b, over_tail, plus_ref, minus_ref):
    rows = down_a.shape[0]
    plus_ref[:rows] = (down_a[...] + over_head[...].astype(F32)).astype(BF16)
    plus_ref[rows:] = down_b[...]
    minus_ref[:rows] = up_a[...]
    minus_ref[rows:] = (up_b[...] + over_tail[...].astype(F32)).astype(BF16)


def back_kernel(total_ref, own_ref, tail_ref, cross_ref, pair_ref, back_ref):
    slots, rest = own_ref.shape[0], tail_ref.shape[0]
    pair = own_ref[...] + cross_ref[:slots].astype(F32)
    tail = tail_ref[...] + cross_ref[slots:].astype(F32)
    pair_ref[...] = pair
    offset = total_ref[0]
    back_ref[...] = (
        picked(slots, slots, offset, pair.astype(BF16))
        + picked(slots, rest, offset - slots, tail.astype(BF16))
    ).astype(BF16)


def grad_kernel(total_ref, raw_ref, own_ref, back_ref, out_ref):
    rows = out_ref.shape[0]
    unit, inverse = unit_rows(raw_ref[...])
    sums = own_ref[...] + back_ref[...].astype(F32)
    grads = (sums - unit * jnp.sum(unit * sums, axis=1, keepdims=True)) * inverse
    slot = pl.program_id(0) * rows + lax.broadcasted_iota(jnp.int32, grads.shape, 0)
    out_ref[...] = jnp.where(slot < total_ref[0], grads, 0.0)


def caption_grads(total, raw, own_rows, back):
    slots, width = raw.shape
    steps = 4
    some = pl.BlockSpec((slots // steps, width), lambda i: (i, 0))
    return pl.pallas_call(
        grad_kernel,
        grid=(steps,),
        out_shape=jax.ShapeDtypeStruct((slots, width), F32),
        in_specs=[SMEM, some, some, some],
        out_specs=some,
        compiler_params=pltpu.CompilerParams(vmem_limit_bytes=16 * MIB),
        cost_estimate=pl.CostEstimate(
            flops=8 * slots * width, bytes_accessed=4 * MIB, transcendentals=0
        ),
        name="caption_grad",
    )(total, raw, own_rows, back)


def program(image_embed, caption_vectors, caption_counts, natural_log_multiplier, match_odds_offset):
    count, width = image_embed.shape
    slots = caption_vectors.shape[0]
    pair_rows = 9 * count
    index = {a: lax.axis_index(a) for a in AXES}
    home = flat([index[a] for a in AXES])
    scale = jnp.exp(natural_log_multiplier[0])
    scalars = jnp.stack([scale, match_odds_offset[0]])

    far_raw = send(image_embed, flip_route(4))
    partner_raw = send(caption_vectors, flip_route(0))

    counts = lax.dynamic_slice_in_dim(caption_counts, home * count, count)
    earlier = lax.iota(jnp.int32, count)[None, :] <= lax.iota(jnp.int32, count)[:, None]
    ends = jnp.sum(jnp.where(earlier, counts[None, :], 0), axis=1, keepdims=True)
    spans = jnp.concatenate([ends - counts[:, None], ends], axis=1)
    total = jnp.sum(counts).reshape(1)

    half = jax.ShapeDtypeStruct((4 * count, width), BF16)
    near = plain(
        near_kernel, jax.ShapeDtypeStruct((2 * count, width), BF16), (image_embed, far_raw)
    )
    first = {}
    for k in (2, 1, 3):
        first[k] = send(near, ring_route(0, k))
    own_pad = plain(
        prep_kernel,
        jax.ShapeDtypeStruct((pair_rows, width), BF16),
        (total, caption_vectors),
        smem=1,
    )
    head, tail = plain(
        join_kernel, (half, half), (near, first[1], first[3], first[2]), after=(own_pad,)
    )
    up_head = send(head, ring_route(1, 1))
    down_tail = send(tail, ring_route(1, 3))
    up_tail = send(tail, ring_route(1, 1))
    down_head = send(head, ring_route(1, 3))
    two_head = send(up_head, ring_route(1, 1))
    two_tail = send(down_tail, ring_route(1, 3))

    own_pair = plain(
        merge_kernel,
        jax.ShapeDtypeStruct((pair_rows, width), BF16),
        (total, own_pad, partner_raw),
        2 * pair_rows * slots * width,
        1,
        after=(head,),
    )
    other_pair = send(own_pair, flip_route(2))
    captions = plain(
        stack_kernel, jax.ShapeDtypeStruct((2 * pair_rows, width), BF16), (own_pair, other_pair)
    )

    def terms(head, tail, types, local=False, after=()):
        return weight_terms(local, types, scalars, spans, head, tail, captions, after)

    w_local, i_local = terms(head, tail, (), True)
    w_down, i_down, down_a, down_b = terms(down_head, down_tail, (F32, BF16), after=(w_local,))
    w_two, i_two, two_a, two_b = terms(two_head, two_tail, (BF16, BF16), after=(down_b,))
    over_head = send(two_a, ring_route(1, 1))
    over_tail = send(two_b, ring_route(1, 3))
    w_up, i_up, up_a, up_b = terms(up_head, up_tail, (BF16, F32), after=(two_a,))
    block_shape = jax.ShapeDtypeStruct((8 * count, width), BF16)
    plus, minus = plain(
        combine_kernel,
        (block_shape, block_shape),
        (down_a, down_b, over_head, up_a, up_b, over_tail),
    )
    below = send(plus, ring_route(1, 1)).astype(F32)
    above = send(minus, ring_route(1, 3)).astype(F32)
    operands = [w_local, w_two, w_down, w_up, i_local, i_two, i_down, i_up]
    sum_flops = 2 * 32 * count * pair_rows * width
    cross, own_tail = plain(
        functools.partial(cross_kernel, 4),
        (
            jax.ShapeDtypeStruct((pair_rows, width), BF16),
            jax.ShapeDtypeStruct((pair_rows - slots, width), F32),
        ),
        operands,
        sum_flops,
        limit=24,
        after=(minus,),
    )
    crossed = send(cross, flip_route(2))
    own_part = plain(
        functools.partial(own_kernel, 4),
        jax.ShapeDtypeStruct((slots, width), F32),
        operands,
        sum_flops,
        limit=24,
        after=(cross,),
    )
    own_rows, back = plain(
        back_kernel,
        (
            jax.ShapeDtypeStruct((slots, width), F32),
            jax.ShapeDtypeStruct((slots, width), BF16),
        ),
        (total, own_part, own_tail, crossed),
        2 * pair_rows * slots * width,
        1,
        24,
    )
    returned = send(back, flip_route(0))
    half_sum = jax.ShapeDtypeStruct((4 * count, width), F32)
    local_a, local_b = plain(
        local_sums_kernel,
        (half_sum, half_sum),
        (w_local, captions),
        16 * count * 2 * pair_rows * width,
        after=(back,),
    )
    rows = 4 * count
    head_sum = local_a + below[:rows] + above[:rows]
    tail_sum = local_b + below[rows:] + above[rows:]

    near_rows = 2 * count
    pieces = {1: head_sum[near_rows:], 3: tail_sum[:near_rows], 2: tail_sum[near_rows:]}
    near_sum = head_sum[:near_rows]
    for k in (2, 1, 3):
        near_sum = near_sum + send(pieces[k].astype(BF16), ring_route(0, -k)).astype(F32)
    far_sum = send(near_sum[count:].astype(BF16), flip_route(4)).astype(F32)
    own_sum = near_sum[:count] + far_sum
    image_unit, image_inverse = unit_rows(image_embed)
    image_grad = (
        own_sum - image_unit * jnp.sum(image_unit * own_sum, axis=1, keepdims=True)
    ) * image_inverse

    caption_grad = caption_grads(total, caption_vectors, own_rows, returned)
    return image_grad, caption_grad


def solution(mesh):
    fine = Mesh(mesh.devices.reshape(SIZES), AXES)
    placed = (P(AXES, None), P(AXES, None), P(), P(), P())
    return jax.shard_map(
        program,
        mesh=fine,
        in_specs=placed,
        out_specs=(P(AXES, None), P(AXES, None)),
        check_vma=False,
    )
```

```python
import functools

import jax
import jax.numpy as jnp
from jax import lax
from jax.experimental import pallas as pl
from jax.experimental.pallas import tpu as pltpu
from jax.sharding import Mesh, PartitionSpec as P


EPSILON = 1e-06
LOG2E = 1.4426950408889634
AXES = ("y_lo", "x", "core", "z", "y_hi")
SIZES = (2, 4, 2, 4, 2)
F32 = jnp.float32
BF16 = jnp.bfloat16
VMEM = pl.BlockSpec(memory_space=pltpu.VMEM)
ANY = pl.BlockSpec(memory_space=pl.ANY)
SMEM = pl.BlockSpec(memory_space=pltpu.SMEM)
MIB = 2**20


def coordinates(device):
    out = []
    for size in reversed(SIZES):
        out.append(device % size)
        device //= size
    return out[::-1]


def flat(coords):
    device = 0
    for size, c in zip(SIZES, coords):
        device = device * size + c
    return device


def route(move):
    pairs = []
    for device in range(128):
        c = coordinates(device)
        move(c)
        pairs.append((device, flat(c)))
    return pairs


def ring_route(stage, distance):
    def move(c):
        axis = 1 if c[2] == stage else 3
        c[axis] = (c[axis] + distance) % 4

    return route(move)


def flip_route(axis):
    def move(c):
        c[axis] = 1 - c[axis]

    return route(move)


def send(value, pairs):
    return lax.ppermute(value, AXES, pairs)


def unit_rows(raw):
    values = raw.astype(F32)
    inverse = lax.rsqrt(jnp.sum(values * values, axis=1, keepdims=True) + EPSILON)
    return values * inverse, inverse


def near_kernel(own_ref, far_ref, near_ref):
    count = own_ref.shape[0]
    near_ref[:count] = unit_rows(own_ref[...])[0].astype(BF16)
    near_ref[count:] = unit_rows(far_ref[...])[0].astype(BF16)


def join_kernel(*refs):
    rows = refs[0].shape[0]
    refs[-2][:rows] = refs[0][...]
    refs[-2][rows:] = refs[1][...]
    refs[-1][:rows] = refs[2][...]
    refs[-1][rows:] = refs[3][...]


def plain(kernel, out_shape, args, flops=10**6, smem=0, limit=16, after=()):
    return pl.pallas_call(
        lambda *refs: kernel(*refs[: len(args)], *refs[len(args) + len(after) :]),
        out_shape=out_shape,
        in_specs=[SMEM] * smem + [VMEM] * (len(args) - smem) + [ANY] * len(after),
        out_specs=(VMEM,) * len(out_shape) if isinstance(out_shape, tuple) else VMEM,
        compiler_params=pltpu.CompilerParams(vmem_limit_bytes=limit * MIB),
        cost_estimate=pl.CostEstimate(flops=flops, bytes_accessed=MIB, transcendentals=0),
    )(*args, *after)


def prep_kernel(total_ref, own_ref, out_ref):
    slots = own_ref.shape[0]
    low = unit_rows(own_ref[...])[0]
    slot = lax.broadcasted_iota(jnp.int32, low.shape, 0)
    out_ref[:slots] = jnp.where(slot < total_ref[0], low, 0.0).astype(BF16)
    out_ref[slots:] = jnp.zeros((out_ref.shape[0] - slots, low.shape[1]), BF16)


def picked(rows, columns, offset, values):
    row = lax.broadcasted_iota(jnp.int32, (rows, columns), 0)
    column = lax.broadcasted_iota(jnp.int32, (rows, columns), 1)
    pick = jnp.where(column == row + offset, 1.0, 0.0).astype(BF16)
    return jnp.dot(pick, values, preferred_element_type=F32)


def merge_kernel(total_ref, own_ref, raw_ref, out_ref):
    low = unit_rows(raw_ref[...])[0].astype(BF16)
    other = picked(out_ref.shape[0], low.shape[0], -total_ref[0], low)
    out_ref[...] = (own_ref[...].astype(F32) + other).astype(BF16)


def stack_kernel(own_ref, other_ref, out_ref):
    rows = own_ref.shape[0]
    out_ref[:512] = own_ref[:512]
    out_ref[512:1024] = other_ref[:512]
    out_ref[1024 : rows + 512] = own_ref[512:]
    out_ref[rows + 512 :] = other_ref[512:]


def weigh(local, scalar_ref, spans_ref, images, captions, weight_ref):
    scale = scalar_ref[0]
    bias = scalar_ref[1]
    scores = lax.dot_general(
        images, captions, (((1,), (1,)), ((), ())), preferred_element_type=F32
    )
    steep = scores * (scale * -LOG2E) + (bias * -LOG2E)
    weight_ref[...] = (scale / (1.0 + jnp.exp2(steep))).astype(BF16)
    if local:
        count = spans_ref.shape[0]
        head = steep[:count, :512]
        slot = lax.broadcasted_iota(jnp.int32, head.shape, 1)
        match = (slot >= spans_ref[:, 0:1]) & (slot < spans_ref[:, 1:2])
        value = scale / (1.0 + jnp.exp2(jnp.where(match, -head, head)))
        weight_ref[:count, :512] = jnp.where(match, -value, value).astype(BF16)


def weight_kernel(
    local, sums, scalar_ref, spans_ref, head_ref, tail_ref, captions_ref, weight_ref, images_ref,
    *outs,
):
    rows = head_ref.shape[0]
    images_ref[:rows] = head_ref[...]
    images_ref[rows:] = tail_ref[...]
    weigh(local, scalar_ref, spans_ref, images_ref[...], captions_ref[...], weight_ref)
    if sums:
        total = jnp.dot(weight_ref[...], captions_ref[...], preferred_element_type=F32)
        outs[0][...] = total[:rows].astype(outs[0].dtype)
        outs[1][...] = total[rows:].astype(outs[1].dtype)


def weight_terms(local, types, scalars, spans, head, tail, captions, after=()):
    rows, width = head.shape
    slots = captions.shape[0]
    arity = 5
    return pl.pallas_call(
        lambda *refs: weight_kernel(
            local, bool(types), *refs[:arity], *refs[arity + len(after) :]
        ),
        out_shape=(
            jax.ShapeDtypeStruct((2 * rows, slots), BF16),
            jax.ShapeDtypeStruct((2 * rows, width), BF16),
            *[jax.ShapeDtypeStruct((rows, width), t) for t in types],
        ),
        in_specs=[SMEM] + [VMEM] * (arity - 1) + [ANY] * len(after),
        out_specs=(VMEM,) * (2 + len(types)),
        compiler_params=pltpu.CompilerParams(vmem_limit_bytes=20 * MIB),
        cost_estimate=pl.CostEstimate(
            flops=(8 if types else 4) * rows * slots * width,
            bytes_accessed=8 * MIB,
            transcendentals=2 * rows * slots,
        ),
        name="block_local" if local else "block_remote",
    )(scalars, spans, head, tail, captions, *after)


def local_sums_kernel(weight_ref, captions_ref, head_out, tail_out):
    rows = head_out.shape[0]
    total = jnp.dot(weight_ref[...], captions_ref[...], preferred_element_type=F32)
    head_out[...] = total[:rows]
    tail_out[...] = total[rows:]


def caption_sum(refs, blocks, columns):
    total = None
    for weight_ref, images_ref in zip(refs[:blocks], refs[blocks : 2 * blocks]):
        part = lax.dot_general(
            weight_ref[:, columns], images_ref[...], (((0,), (0,)), ((), ())),
            preferred_element_type=F32,
        )
        total = part if total is None else total + part
    return total


def cross_kernel(blocks, *refs):
    cross_ref, tail_ref = refs[-2:]
    rest = tail_ref.shape[0]
    total = caption_sum(refs, blocks, slice(512, refs[0].shape[1]))
    cross_ref[:512] = total[:512].astype(BF16)
    tail_ref[...] = total[512 : 512 + rest]
    cross_ref[512:] = total[512 + rest :].astype(BF16)


def own_kernel(blocks, *refs):
    refs[-1][...] = caption_sum(refs, blocks, slice(0, 512))


def combine_kernel(down_a, down_b, over_head, up_a, up_b, over_tail, plus_ref, minus_ref):
    rows = down_a.shape[0]
    plus_ref[:rows] = (down_a[...] + over_head[...].astype(F32)).astype(BF16)
    plus_ref[rows:] = down_b[...]
    minus_ref[:rows] = up_a[...]
    minus_ref[rows:] = (up_b[...] + over_tail[...].astype(F32)).astype(BF16)


def back_kernel(own_ref, tail_ref, cross_ref, pair_ref, back_a, back_b):
    slots, rest = own_ref.shape[0], tail_ref.shape[0]
    pair = own_ref[...] + cross_ref[:slots].astype(F32)
    tail = tail_ref[...] + cross_ref[slots:].astype(F32)
    first = back_a.shape[0]
    pair_ref[...] = pair
    back_a[...] = pair[rest : rest + first].astype(BF16)
    back_b[: slots - rest - first] = pair[rest + first :].astype(BF16)
    back_b[slots - rest - first :] = tail.astype(BF16)


def home_kernel(total_ref, own_ref, back_ref, out_ref):
    slots = own_ref.shape[0]
    out_ref[...] = own_ref[...] + picked(
        slots, back_ref.shape[0], slots - total_ref[0], back_ref[...]
    )


def grad_kernel(skip, total_ref, raw_ref, own_ref, back_ref, out_ref):
    rows = out_ref.shape[0]
    start = pl.program_id(0) * rows
    unit, inverse = unit_rows(raw_ref[...])
    offset = start + pl.num_programs(0) * rows - total_ref[0] - skip
    sums = own_ref[...] + picked(rows, back_ref.shape[0], offset, back_ref[...])
    grads = (sums - unit * jnp.sum(unit * sums, axis=1, keepdims=True)) * inverse
    slot = start + lax.broadcasted_iota(jnp.int32, grads.shape, 0)
    out_ref[...] = jnp.where(slot < total_ref[0], grads, 0.0)


def caption_grads(skip, total, raw, own_rows, back):
    slots, width = raw.shape
    steps = 4
    some = pl.BlockSpec((slots // steps, width), lambda i: (i, 0))
    return pl.pallas_call(
        functools.partial(grad_kernel, skip),
        grid=(steps,),
        out_shape=jax.ShapeDtypeStruct((slots, width), F32),
        in_specs=[SMEM, some, some, pl.BlockSpec(back.shape, lambda i: (0, 0))],
        out_specs=some,
        compiler_params=pltpu.CompilerParams(vmem_limit_bytes=16 * MIB),
        cost_estimate=pl.CostEstimate(
            flops=8 * slots * width, bytes_accessed=4 * MIB, transcendentals=0
        ),
        name="caption_grad",
    )(total, raw, own_rows, back)


def program(image_embed, caption_vectors, caption_counts, natural_log_multiplier, match_odds_offset):
    count, width = image_embed.shape
    slots = caption_vectors.shape[0]
    pair_rows = 9 * count
    index = {a: lax.axis_index(a) for a in AXES}
    home = flat([index[a] for a in AXES])
    scale = jnp.exp(natural_log_multiplier[0])
    scalars = jnp.stack([scale, match_odds_offset[0]])

    far_raw = send(image_embed, flip_route(4))
    partner_raw = send(caption_vectors, flip_route(0))

    counts = lax.dynamic_slice_in_dim(caption_counts, home * count, count)
    earlier = lax.iota(jnp.int32, count)[None, :] <= lax.iota(jnp.int32, count)[:, None]
    ends = jnp.sum(jnp.where(earlier, counts[None, :], 0), axis=1, keepdims=True)
    spans = jnp.concatenate([ends - counts[:, None], ends], axis=1)
    total = jnp.sum(counts).reshape(1)

    half = jax.ShapeDtypeStruct((4 * count, width), BF16)
    near = plain(
        near_kernel, jax.ShapeDtypeStruct((2 * count, width), BF16), (image_embed, far_raw)
    )
    first = {}
    for k in (2, 1, 3):
        first[k] = send(near, ring_route(0, k))
    own_pad = plain(
        prep_kernel,
        jax.ShapeDtypeStruct((pair_rows, width), BF16),
        (total, caption_vectors),
        smem=1,
    )
    head, tail = plain(
        join_kernel, (half, half), (near, first[1], first[3], first[2]), after=(own_pad,)
    )
    up_head = send(head, ring_route(1, 1))
    down_tail = send(tail, ring_route(1, 3))
    up_tail = send(tail, ring_route(1, 1))
    down_head = send(head, ring_route(1, 3))
    two_head = send(up_head, ring_route(1, 1))
    two_tail = send(down_tail, ring_route(1, 3))

    own_pair = plain(
        merge_kernel,
        jax.ShapeDtypeStruct((pair_rows, width), BF16),
        (total, own_pad, partner_raw),
        2 * pair_rows * slots * width,
        1,
        after=(head,),
    )
    other_pair = send(own_pair, flip_route(2))
    captions = plain(
        stack_kernel, jax.ShapeDtypeStruct((2 * pair_rows, width), BF16), (own_pair, other_pair)
    )

    def terms(head, tail, types, local=False, after=()):
        return weight_terms(local, types, scalars, spans, head, tail, captions, after)

    w_local, i_local = terms(head, tail, (), True)
    w_down, i_down, down_a, down_b = terms(down_head, down_tail, (F32, BF16), after=(w_local,))
    w_two, i_two, two_a, two_b = terms(two_head, two_tail, (BF16, BF16), after=(down_b,))
    over_head = send(two_a, ring_route(1, 1))
    over_tail = send(two_b, ring_route(1, 3))
    w_up, i_up, up_a, up_b = terms(up_head, up_tail, (BF16, F32), after=(two_a,))
    operands = [w_local, w_two, w_down, w_up, i_local, i_two, i_down, i_up]
    sum_flops = 2 * 32 * count * pair_rows * width
    cross, own_tail = plain(
        functools.partial(cross_kernel, 4),
        (
            jax.ShapeDtypeStruct((pair_rows, width), BF16),
            jax.ShapeDtypeStruct((pair_rows - slots, width), F32),
        ),
        operands,
        sum_flops,
        limit=24,
        after=(up_a,),
    )
    crossed = send(cross, flip_route(2))
    block_shape = jax.ShapeDtypeStruct((8 * count, width), BF16)
    plus, minus = plain(
        combine_kernel,
        (block_shape, block_shape),
        (down_a, down_b, over_head, up_a, up_b, over_tail),
        after=(cross,),
    )
    below = send(plus, ring_route(1, 1)).astype(F32)
    above = send(minus, ring_route(1, 3)).astype(F32)
    own_part = plain(
        functools.partial(own_kernel, 4),
        jax.ShapeDtypeStruct((slots, width), F32),
        operands,
        sum_flops,
        limit=24,
        after=(minus,),
    )
    last = slots // 4
    pair, back_a, back_b = plain(
        back_kernel,
        (
            jax.ShapeDtypeStruct((slots, width), F32),
            jax.ShapeDtypeStruct((slots - last, width), BF16),
            jax.ShapeDtypeStruct((last, width), BF16),
        ),
        (own_part, own_tail, crossed),
        limit=24,
    )
    returned_a = send(back_a, flip_route(0))
    returned_b = send(back_b, flip_route(0))
    half_sum = jax.ShapeDtypeStruct((4 * count, width), F32)
    local_a, local_b = plain(
        local_sums_kernel,
        (half_sum, half_sum),
        (w_local, captions),
        16 * count * 2 * pair_rows * width,
        after=(back_a,),
    )
    rows = 4 * count
    head_sum = local_a + below[:rows] + above[:rows]
    tail_sum = local_b + below[rows:] + above[rows:]

    near_rows = 2 * count
    pieces = {1: head_sum[near_rows:], 3: tail_sum[:near_rows], 2: tail_sum[near_rows:]}
    near_sum = head_sum[:near_rows]
    for k in (2, 1, 3):
        near_sum = near_sum + send(pieces[k].astype(BF16), ring_route(0, -k)).astype(F32)
    far_sum = send(near_sum[count:].astype(BF16), flip_route(4)).astype(F32)
    own_sum = near_sum[:count] + far_sum
    image_unit, image_inverse = unit_rows(image_embed)
    image_grad = (
        own_sum - image_unit * jnp.sum(image_unit * own_sum, axis=1, keepdims=True)
    ) * image_inverse

    own_rows = plain(
        home_kernel,
        jax.ShapeDtypeStruct((slots, width), F32),
        (total, pair, returned_a),
        2 * slots * slots * width,
        1,
    )
    caption_grad = caption_grads(slots - last, total, caption_vectors, own_rows, returned_b)
    return image_grad, caption_grad


def solution(mesh):
    fine = Mesh(mesh.devices.reshape(SIZES), AXES)
    placed = (P(AXES, None), P(AXES, None), P(), P(), P())
    return jax.shard_map(
        program,
        mesh=fine,
        in_specs=placed,
        out_specs=(P(AXES, None), P(AXES, None)),
        check_vma=False,
    )
```

```python
import functools

import jax
import jax.numpy as jnp
from jax import lax
from jax.experimental import pallas as pl
from jax.experimental.pallas import tpu as pltpu
from jax.sharding import Mesh, PartitionSpec as P


EPSILON = 1e-06
LOG2E = 1.4426950408889634
AXES = ("y_lo", "x", "core", "z", "y_hi")
SIZES = (2, 4, 2, 4, 2)
F32 = jnp.float32
BF16 = jnp.bfloat16
VMEM = pl.BlockSpec(memory_space=pltpu.VMEM)
ANY = pl.BlockSpec(memory_space=pl.ANY)
SMEM = pl.BlockSpec(memory_space=pltpu.SMEM)
MIB = 2**20


def coordinates(device):
    out = []
    for size in reversed(SIZES):
        out.append(device % size)
        device //= size
    return out[::-1]


def flat(coords):
    device = 0
    for size, c in zip(SIZES, coords):
        device = device * size + c
    return device


def route(move):
    pairs = []
    for device in range(128):
        c = coordinates(device)
        move(c)
        pairs.append((device, flat(c)))
    return pairs


def ring_route(stage, distance):
    def move(c):
        axis = 1 if c[2] == stage else 3
        c[axis] = (c[axis] + distance) % 4

    return route(move)


def flip_route(*axes):
    def move(c):
        for axis in axes:
            c[axis] = 1 - c[axis]

    return route(move)


def send(value, pairs):
    return lax.ppermute(value, AXES, pairs)


def unit_rows(raw):
    values = raw.astype(F32)
    inverse = lax.rsqrt(jnp.sum(values * values, axis=1, keepdims=True) + EPSILON)
    return values * inverse, inverse


def low_kernel(raw_ref, out_ref):
    out_ref[...] = unit_rows(raw_ref[...])[0].astype(BF16)


def near_kernel(own_ref, far_ref, near_ref):
    count = own_ref.shape[0]
    near_ref[:count] = own_ref[...]
    near_ref[count:] = unit_rows(far_ref[...])[0].astype(BF16)


def join_kernel(*refs):
    rows = refs[0].shape[0]
    refs[-2][:rows] = refs[0][...]
    refs[-2][rows:] = refs[1][...]
    refs[-1][:rows] = refs[2][...]
    refs[-1][rows:] = refs[3][...]


def plain(kernel, out_shape, args, flops=10**6, smem=0, limit=16, after=()):
    return pl.pallas_call(
        lambda *refs: kernel(*refs[: len(args)], *refs[len(args) + len(after) :]),
        out_shape=out_shape,
        in_specs=[SMEM] * smem + [VMEM] * (len(args) - smem) + [ANY] * len(after),
        out_specs=(VMEM,) * len(out_shape) if isinstance(out_shape, tuple) else VMEM,
        compiler_params=pltpu.CompilerParams(vmem_limit_bytes=limit * MIB),
        cost_estimate=pl.CostEstimate(flops=flops, bytes_accessed=MIB, transcendentals=0),
    )(*args, *after)


def prep_kernel(total_ref, own_ref, out_ref):
    slots = own_ref.shape[0]
    low = unit_rows(own_ref[...])[0]
    slot = lax.broadcasted_iota(jnp.int32, low.shape, 0)
    out_ref[:slots] = jnp.where(slot < total_ref[0], low, 0.0).astype(BF16)
    out_ref[slots:] = jnp.zeros((out_ref.shape[0] - slots, low.shape[1]), BF16)


def picked(rows, columns, offset, values):
    row = lax.broadcasted_iota(jnp.int32, (rows, columns), 0)
    column = lax.broadcasted_iota(jnp.int32, (rows, columns), 1)
    pick = jnp.where(column == row + offset, 1.0, 0.0).astype(BF16)
    return jnp.dot(pick, values, preferred_element_type=F32)


def merge_kernel(total_ref, own_ref, raw_ref, out_ref):
    low = unit_rows(raw_ref[...])[0].astype(BF16)
    other = picked(out_ref.shape[0], low.shape[0], -total_ref[0], low)
    out_ref[...] = (own_ref[...].astype(F32) + other).astype(BF16)


def stack_kernel(own_ref, other_ref, out_ref):
    rows = own_ref.shape[0]
    out_ref[:512] = own_ref[:512]
    out_ref[512:1024] = other_ref[:512]
    out_ref[1024 : rows + 512] = own_ref[512:]
    out_ref[rows + 512 :] = other_ref[512:]


def weigh(local, scalar_ref, spans_ref, images, captions, weight_ref):
    scale = scalar_ref[0]
    bias = scalar_ref[1]
    scores = lax.dot_general(
        images, captions, (((1,), (1,)), ((), ())), preferred_element_type=F32
    )
    steep = scores * (scale * -LOG2E) + (bias * -LOG2E)
    weight_ref[...] = (scale / (1.0 + jnp.exp2(steep))).astype(BF16)
    if local:
        count = spans_ref.shape[0]
        head = steep[:count, :512]
        slot = lax.broadcasted_iota(jnp.int32, head.shape, 1)
        match = (slot >= spans_ref[:, 0:1]) & (slot < spans_ref[:, 1:2])
        value = scale / (1.0 + jnp.exp2(jnp.where(match, -head, head)))
        weight_ref[:count, :512] = jnp.where(match, -value, value).astype(BF16)


def weight_kernel(
    local, sums, scalar_ref, spans_ref, head_ref, tail_ref, captions_ref, weight_ref, images_ref,
    *outs,
):
    rows = head_ref.shape[0]
    images_ref[:rows] = head_ref[...]
    images_ref[rows:] = tail_ref[...]
    weigh(local, scalar_ref, spans_ref, images_ref[...], captions_ref[...], weight_ref)
    if sums:
        total = jnp.dot(weight_ref[...], captions_ref[...], preferred_element_type=F32)
        outs[0][...] = total[:rows].astype(outs[0].dtype)
        outs[1][...] = total[rows:].astype(outs[1].dtype)


def weight_terms(local, types, scalars, spans, head, tail, captions, after=()):
    rows, width = head.shape
    slots = captions.shape[0]
    arity = 5
    return pl.pallas_call(
        lambda *refs: weight_kernel(
            local, bool(types), *refs[:arity], *refs[arity + len(after) :]
        ),
        out_shape=(
            jax.ShapeDtypeStruct((2 * rows, slots), BF16),
            jax.ShapeDtypeStruct((2 * rows, width), BF16),
            *[jax.ShapeDtypeStruct((rows, width), t) for t in types],
        ),
        in_specs=[SMEM] + [VMEM] * (arity - 1) + [ANY] * len(after),
        out_specs=(VMEM,) * (2 + len(types)),
        compiler_params=pltpu.CompilerParams(vmem_limit_bytes=20 * MIB),
        cost_estimate=pl.CostEstimate(
            flops=(8 if types else 4) * rows * slots * width,
            bytes_accessed=8 * MIB,
            transcendentals=2 * rows * slots,
        ),
        name="block_local" if local else "block_remote",
    )(scalars, spans, head, tail, captions, *after)


def local_sums_kernel(weight_ref, captions_ref, head_out, tail_out):
    rows = head_out.shape[0]
    total = jnp.dot(weight_ref[...], captions_ref[...], preferred_element_type=F32)
    head_out[...] = total[:rows]
    tail_out[...] = total[rows:]


def caption_sum(refs, blocks, columns):
    total = None
    for weight_ref, images_ref in zip(refs[:blocks], refs[blocks : 2 * blocks]):
        part = lax.dot_general(
            weight_ref[:, columns], images_ref[...], (((0,), (0,)), ((), ())),
            preferred_element_type=F32,
        )
        total = part if total is None else total + part
    return total


def cross_kernel(blocks, *refs):
    cross_ref, tail_ref = refs[-2:]
    rest = tail_ref.shape[0]
    total = caption_sum(refs, blocks, slice(512, refs[0].shape[1]))
    cross_ref[:512] = total[:512].astype(BF16)
    tail_ref[...] = total[512 : 512 + rest]
    cross_ref[512:] = total[512 + rest :].astype(BF16)


def own_kernel(blocks, *refs):
    refs[-1][...] = caption_sum(refs, blocks, slice(0, 512))


def combine_kernel(down_a, down_b, over_head, up_a, up_b, over_tail, plus_ref, minus_ref):
    rows = down_a.shape[0]
    plus_ref[:rows] = (down_a[...] + over_head[...].astype(F32)).astype(BF16)
    plus_ref[rows:] = down_b[...]
    minus_ref[:rows] = up_a[...]
    minus_ref[rows:] = (up_b[...] + over_tail[...].astype(F32)).astype(BF16)


def back_kernel(own_ref, tail_ref, cross_ref, pair_ref, back_a, back_b):
    slots, rest = own_ref.shape[0], tail_ref.shape[0]
    pair = own_ref[...] + cross_ref[:slots].astype(F32)
    tail = tail_ref[...] + cross_ref[slots:].astype(F32)
    first = back_a.shape[0]
    pair_ref[...] = pair
    back_a[...] = pair[rest : rest + first].astype(BF16)
    back_b[: slots - rest - first] = pair[rest + first :].astype(BF16)
    back_b[slots - rest - first :] = tail.astype(BF16)


def image_kernel(raw_ref, own_ref, a_ref, b_ref, c_ref, far_ref, out_ref):
    count = own_ref.shape[0]
    sums = own_ref[...] + a_ref[:count].astype(F32) + b_ref[:count].astype(F32)
    sums = sums + c_ref[:count].astype(F32) + far_ref[...].astype(F32)
    out_ref[...] = project(raw_ref[...], sums)


def project(raw, sums):
    unit, inverse = unit_rows(raw)
    return (sums - unit * jnp.sum(unit * sums, axis=1, keepdims=True)) * inverse


def window_start(total, last, rows, slots):
    return pl.multiple_of(jnp.clip((total - last) // 16 * 16, 0, slots - rows), 16)


def home_kernel(
    last, total_ref, raw_ref, own_ref, back_ref, out_ref, part_raw, part_sums, sums_ref, grads_ref,
    sems,
):
    slots = own_ref.shape[0]
    rows = part_raw.shape[0]
    total = total_ref[0]
    steps = sems.shape[0]
    tile = slots // steps
    copies = []
    for step in range(steps):
        part = slice(step * tile, (step + 1) * tile)
        offset = slots - total + step * tile
        sums = own_ref[part] + picked(tile, back_ref.shape[0], offset, back_ref[...])
        sums_ref[part] = sums
        slot = step * tile + lax.broadcasted_iota(jnp.int32, sums.shape, 0)
        grads_ref[part] = jnp.where(slot < total, project(raw_ref[part], sums), 0.0)
        copies.append(
            pltpu.make_async_copy(grads_ref.at[part], out_ref.at[part], sems.at[step])
        )
        copies[-1].start()
    window = pl.ds(window_start(total, last, rows, slots), rows)
    part_raw[...] = raw_ref[window, :]
    part_sums[...] = sums_ref[window, :]
    for copy in copies:
        copy.wait()


def last_kernel(total_ref, raw_ref, sums_ref, back_ref, early_ref, out_ref, grads_ref, sem):
    last, rows = back_ref.shape[0], grads_ref.shape[0]
    total = total_ref[0]
    start = window_start(total, last, rows, out_ref.shape[0])
    sums = sums_ref[...] + picked(rows, last, start + last - total, back_ref[...])
    slot = start + lax.broadcasted_iota(jnp.int32, sums.shape, 0)
    grads_ref[...] = jnp.where(slot < total, project(raw_ref[...], sums), 0.0)
    copy = pltpu.make_async_copy(grads_ref, out_ref.at[pl.ds(start, rows), :], sem)
    copy.start()
    copy.wait()


def caption_grads(total, raw, own, back, last):
    slots, width = raw.shape
    rows = last + 16
    return pl.pallas_call(
        functools.partial(home_kernel, last),
        out_shape=(
            jax.ShapeDtypeStruct((slots, width), F32),
            jax.ShapeDtypeStruct((rows, width), BF16),
            jax.ShapeDtypeStruct((rows, width), F32),
        ),
        in_specs=[SMEM, VMEM, VMEM, VMEM],
        out_specs=(ANY, VMEM, VMEM),
        scratch_shapes=[
            pltpu.VMEM((slots, width), F32),
            pltpu.VMEM((slots, width), F32),
            pltpu.SemaphoreType.DMA((4,)),
        ],
        compiler_params=pltpu.CompilerParams(vmem_limit_bytes=20 * MIB),
        cost_estimate=pl.CostEstimate(
            flops=2 * slots * slots * width, bytes_accessed=8 * MIB, transcendentals=0
        ),
        name="caption_grad",
    )(total, raw, own, back)


def last_rows(total, raw, sums, back, early):
    slots, width = early.shape
    return pl.pallas_call(
        last_kernel,
        out_shape=jax.ShapeDtypeStruct((slots, width), F32),
        in_specs=[SMEM, VMEM, VMEM, VMEM, ANY],
        out_specs=ANY,
        scratch_shapes=[pltpu.VMEM(sums.shape, F32), pltpu.SemaphoreType.DMA],
        input_output_aliases={4: 0},
        compiler_params=pltpu.CompilerParams(vmem_limit_bytes=8 * MIB),
        cost_estimate=pl.CostEstimate(flops=10**6, bytes_accessed=MIB, transcendentals=0),
        name="caption_grad_last",
    )(total, raw, sums, back, early)


def program(image_embed, caption_vectors, caption_counts, natural_log_multiplier, match_odds_offset):
    count, width = image_embed.shape
    slots = caption_vectors.shape[0]
    pair_rows = 9 * count
    index = {a: lax.axis_index(a) for a in AXES}
    home = flat([index[a] for a in AXES])
    scale = jnp.exp(natural_log_multiplier[0])
    scalars = jnp.stack([scale, match_odds_offset[0]])

    partner_raw = send(caption_vectors, flip_route(0))
    far_raw = send(image_embed, flip_route(0, 4))

    counts = lax.dynamic_slice_in_dim(caption_counts, home * count, count)
    earlier = lax.iota(jnp.int32, count)[None, :] <= lax.iota(jnp.int32, count)[:, None]
    ends = jnp.sum(jnp.where(earlier, counts[None, :], 0), axis=1, keepdims=True)
    spans = jnp.concatenate([ends - counts[:, None], ends], axis=1)
    total = jnp.sum(counts).reshape(1)

    half = jax.ShapeDtypeStruct((4 * count, width), BF16)
    own_low = plain(low_kernel, jax.ShapeDtypeStruct((count, width), BF16), (image_embed,), limit=4)
    near = plain(
        near_kernel, jax.ShapeDtypeStruct((2 * count, width), BF16), (own_low, far_raw), limit=4
    )
    first = {}
    for k in (2, 1, 3):
        first[k] = send(near, ring_route(0, k))
    own_pad = plain(
        prep_kernel,
        jax.ShapeDtypeStruct((pair_rows, width), BF16),
        (total, caption_vectors),
        smem=1,
    )
    head, tail = plain(
        join_kernel, (half, half), (near, first[1], first[3], first[2]), after=(own_pad,)
    )
    up_head = send(head, ring_route(1, 1))
    down_tail = send(tail, ring_route(1, 3))
    up_tail = send(tail, ring_route(1, 1))
    down_head = send(head, ring_route(1, 3))
    two_head = send(up_head, ring_route(1, 1))
    two_tail = send(down_tail, ring_route(1, 3))

    own_pair = plain(
        merge_kernel,
        jax.ShapeDtypeStruct((pair_rows, width), BF16),
        (total, own_pad, partner_raw),
        2 * pair_rows * slots * width,
        1,
        after=(head,),
    )
    other_pair = send(own_pair, flip_route(2))
    captions = plain(
        stack_kernel, jax.ShapeDtypeStruct((2 * pair_rows, width), BF16), (own_pair, other_pair)
    )

    def terms(head, tail, types, local=False, after=()):
        return weight_terms(local, types, scalars, spans, head, tail, captions, after)

    w_local, i_local = terms(head, tail, (), True)
    w_down, i_down, down_a, down_b = terms(down_head, down_tail, (F32, BF16), after=(w_local,))
    w_two, i_two, two_a, two_b = terms(two_head, two_tail, (BF16, BF16), after=(down_b,))
    over_head = send(two_a, ring_route(1, 1))
    over_tail = send(two_b, ring_route(1, 3))
    w_up, i_up, up_a, up_b = terms(up_head, up_tail, (BF16, F32), after=(two_a,))
    operands = [w_local, w_two, w_down, w_up, i_local, i_two, i_down, i_up]
    sum_flops = 2 * 32 * count * pair_rows * width
    cross, own_tail = plain(
        functools.partial(cross_kernel, 4),
        (
            jax.ShapeDtypeStruct((pair_rows, width), BF16),
            jax.ShapeDtypeStruct((pair_rows - slots, width), F32),
        ),
        operands,
        sum_flops,
        limit=24,
        after=(up_a,),
    )
    crossed = send(cross, flip_route(2))
    block_shape = jax.ShapeDtypeStruct((8 * count, width), BF16)
    plus, minus = plain(
        combine_kernel,
        (block_shape, block_shape),
        (down_a, down_b, over_head, up_a, up_b, over_tail),
        after=(cross,),
    )
    below = send(plus, ring_route(1, 1)).astype(F32)
    above = send(minus, ring_route(1, 3)).astype(F32)
    own_part = plain(
        functools.partial(own_kernel, 4),
        jax.ShapeDtypeStruct((slots, width), F32),
        operands,
        sum_flops,
        limit=24,
        after=(minus,),
    )
    last = 3 * slots // 8
    pair, back_a, back_b = plain(
        back_kernel,
        (
            jax.ShapeDtypeStruct((slots, width), F32),
            jax.ShapeDtypeStruct((slots - last, width), BF16),
            jax.ShapeDtypeStruct((last, width), BF16),
        ),
        (own_part, own_tail, crossed),
        limit=24,
    )
    returned_a = send(back_a, flip_route(0))
    returned_b = send(back_b, flip_route(0))
    half_sum = jax.ShapeDtypeStruct((4 * count, width), F32)
    local_a, local_b = plain(
        local_sums_kernel,
        (half_sum, half_sum),
        (w_local, captions),
        16 * count * 2 * pair_rows * width,
        after=(back_a,),
    )
    rows = 4 * count
    head_sum = local_a + below[:rows] + above[:rows]
    tail_sum = local_b + below[rows:] + above[rows:]

    near_rows = 2 * count
    pieces = {1: head_sum[near_rows:], 3: tail_sum[:near_rows], 2: tail_sum[near_rows:]}
    far_sum = head_sum[count:near_rows]
    near_back = []
    for k in (2, 1, 3):
        near_back.append(send(pieces[k].astype(BF16), ring_route(0, -k)))
        far_sum = far_sum + near_back[-1][count:].astype(F32)
    far_back = send(far_sum.astype(BF16), flip_route(0, 4))
    early_grad, part_raw, part_sums = caption_grads(total, caption_vectors, pair, returned_a, last)
    image_grad = plain(
        image_kernel,
        jax.ShapeDtypeStruct((count, width), F32),
        (image_embed, head_sum[:count], *near_back, far_back),
        limit=8,
    )
    caption_grad = last_rows(total, part_raw, part_sums, returned_b, early_grad)
    return image_grad, caption_grad


def solution(mesh):
    fine = Mesh(mesh.devices.reshape(SIZES), AXES)
    placed = (P(AXES, None), P(AXES, None), P(), P(), P())
    return jax.shard_map(
        program,
        mesh=fine,
        in_specs=placed,
        out_specs=(P(AXES, None), P(AXES, None)),
        check_vma=False,
    )
```

```python
import functools

import jax
import jax.numpy as jnp
from jax import lax
from jax.experimental import pallas as pl
from jax.experimental.pallas import tpu as pltpu
from jax.sharding import Mesh, PartitionSpec as P


EPSILON = 1e-06
LOG2E = 1.4426950408889634
AXES = ("y_lo", "x", "core", "z", "y_hi")
SIZES = (2, 4, 2, 4, 2)
F32 = jnp.float32
BF16 = jnp.bfloat16
VMEM = pl.BlockSpec(memory_space=pltpu.VMEM)
ANY = pl.BlockSpec(memory_space=pl.ANY)
SMEM = pl.BlockSpec(memory_space=pltpu.SMEM)
MIB = 2**20


def coordinates(device):
    out = []
    for size in reversed(SIZES):
        out.append(device % size)
        device //= size
    return out[::-1]


def flat(coords):
    device = 0
    for size, c in zip(SIZES, coords):
        device = device * size + c
    return device


def route(move):
    pairs = []
    for device in range(128):
        c = coordinates(device)
        move(c)
        pairs.append((device, flat(c)))
    return pairs


def ring_route(stage, distance):
    def move(c):
        axis = 1 if c[2] == stage else 3
        c[axis] = (c[axis] + distance) % 4

    return route(move)


def flip_route(*axes):
    def move(c):
        for axis in axes:
            c[axis] = 1 - c[axis]

    return route(move)


def send(value, pairs):
    return lax.ppermute(value, AXES, pairs)


def unit_rows(raw):
    values = raw.astype(F32)
    inverse = lax.rsqrt(jnp.sum(values * values, axis=1, keepdims=True) + EPSILON)
    return values * inverse, inverse


def low_kernel(raw_ref, out_ref):
    out_ref[...] = unit_rows(raw_ref[...])[0].astype(BF16)


def near_kernel(own_ref, far_ref, near_ref):
    count = own_ref.shape[0]
    near_ref[:count] = own_ref[...]
    near_ref[count:] = unit_rows(far_ref[...])[0].astype(BF16)


def join_kernel(*refs):
    rows = refs[0].shape[0]
    refs[-2][:rows] = refs[0][...]
    refs[-2][rows:] = refs[1][...]
    refs[-1][:rows] = refs[2][...]
    refs[-1][rows:] = refs[3][...]


def plain(kernel, out_shape, args, flops=10**6, smem=0, limit=16, after=()):
    return pl.pallas_call(
        lambda *refs: kernel(*refs[: len(args)], *refs[len(args) + len(after) :]),
        out_shape=out_shape,
        in_specs=[SMEM] * smem + [VMEM] * (len(args) - smem) + [ANY] * len(after),
        out_specs=(VMEM,) * len(out_shape) if isinstance(out_shape, tuple) else VMEM,
        compiler_params=pltpu.CompilerParams(vmem_limit_bytes=limit * MIB),
        cost_estimate=pl.CostEstimate(flops=flops, bytes_accessed=MIB, transcendentals=0),
    )(*args, *after)


def prep_kernel(total_ref, own_ref, out_ref, pick_ref):
    slots = own_ref.shape[0]
    low = unit_rows(own_ref[...])[0]
    slot = lax.broadcasted_iota(jnp.int32, low.shape, 0)
    out_ref[:slots] = jnp.where(slot < total_ref[0], low, 0.0).astype(BF16)
    out_ref[slots:] = jnp.zeros((out_ref.shape[0] - slots, low.shape[1]), BF16)
    row = lax.broadcasted_iota(jnp.int32, pick_ref.shape, 0)
    column = lax.broadcasted_iota(jnp.int32, pick_ref.shape, 1)
    pick_ref[...] = jnp.where(column == row - total_ref[0], 1.0, 0.0).astype(BF16)


def picked(rows, columns, offset, values):
    row = lax.broadcasted_iota(jnp.int32, (rows, columns), 0)
    column = lax.broadcasted_iota(jnp.int32, (rows, columns), 1)
    pick = jnp.where(column == row + offset, 1.0, 0.0).astype(BF16)
    return jnp.dot(pick, values, preferred_element_type=F32)


def merge_kernel(own_ref, pick_ref, raw_ref, out_ref):
    low = unit_rows(raw_ref[...])[0].astype(BF16)
    other = jnp.dot(pick_ref[...], low, preferred_element_type=F32).astype(BF16)
    out_ref[...] = own_ref[...] + other


def stack_kernel(own_ref, other_ref, out_ref):
    rows = own_ref.shape[0]
    out_ref[:512] = own_ref[:512]
    out_ref[512:1024] = other_ref[:512]
    out_ref[1024 : rows + 512] = own_ref[512:]
    out_ref[rows + 512 :] = other_ref[512:]


def weigh(local, scalar_ref, spans_ref, images, captions, weight_ref):
    scale = scalar_ref[0]
    bias = scalar_ref[1]
    scores = lax.dot_general(
        images, captions, (((1,), (1,)), ((), ())), preferred_element_type=F32
    )
    steep = scores * (scale * -LOG2E) + (bias * -LOG2E)
    weight_ref[...] = (scale / (1.0 + jnp.exp2(steep))).astype(BF16)
    if local:
        count = spans_ref.shape[0]
        head = steep[:count, :512]
        slot = lax.broadcasted_iota(jnp.int32, head.shape, 1)
        match = (slot >= spans_ref[:, 0:1]) & (slot < spans_ref[:, 1:2])
        value = scale / (1.0 + jnp.exp2(jnp.where(match, -head, head)))
        weight_ref[:count, :512] = jnp.where(match, -value, value).astype(BF16)


def weight_kernel(
    local, sums, scalar_ref, spans_ref, head_ref, tail_ref, captions_ref, weight_ref, images_ref,
    *outs,
):
    rows = head_ref.shape[0]
    images_ref[:rows] = head_ref[...]
    images_ref[rows:] = tail_ref[...]
    weigh(local, scalar_ref, spans_ref, images_ref[...], captions_ref[...], weight_ref)
    if sums:
        total = jnp.dot(weight_ref[...], captions_ref[...], preferred_element_type=F32)
        outs[0][...] = total[:rows].astype(outs[0].dtype)
        outs[1][...] = total[rows:].astype(outs[1].dtype)


def weight_terms(local, types, scalars, spans, head, tail, captions, after=()):
    rows, width = head.shape
    slots = captions.shape[0]
    arity = 5
    return pl.pallas_call(
        lambda *refs: weight_kernel(
            local, bool(types), *refs[:arity], *refs[arity + len(after) :]
        ),
        out_shape=(
            jax.ShapeDtypeStruct((2 * rows, slots), BF16),
            jax.ShapeDtypeStruct((2 * rows, width), BF16),
            *[jax.ShapeDtypeStruct((rows, width), t) for t in types],
        ),
        in_specs=[SMEM] + [VMEM] * (arity - 1) + [ANY] * len(after),
        out_specs=(VMEM,) * (2 + len(types)),
        compiler_params=pltpu.CompilerParams(vmem_limit_bytes=20 * MIB),
        cost_estimate=pl.CostEstimate(
            flops=(8 if types else 4) * rows * slots * width,
            bytes_accessed=8 * MIB,
            transcendentals=2 * rows * slots,
        ),
        name="block_local" if local else "block_remote",
    )(scalars, spans, head, tail, captions, *after)


def local_sums_kernel(weight_ref, captions_ref, head_out, tail_out):
    rows = head_out.shape[0]
    total = jnp.dot(weight_ref[...], captions_ref[...], preferred_element_type=F32)
    head_out[...] = total[:rows]
    tail_out[...] = total[rows:]


def caption_sum(refs, blocks, columns):
    total = None
    for weight_ref, images_ref in zip(refs[:blocks], refs[blocks : 2 * blocks]):
        part = lax.dot_general(
            weight_ref[:, columns], images_ref[...], (((0,), (0,)), ((), ())),
            preferred_element_type=F32,
        )
        total = part if total is None else total + part
    return total


def cross_kernel(blocks, *refs):
    cross_ref, tail_ref = refs[-2:]
    rest = tail_ref.shape[0]
    total = caption_sum(refs, blocks, slice(512, refs[0].shape[1]))
    cross_ref[:512] = total[:512].astype(BF16)
    tail_ref[...] = total[512 : 512 + rest]
    cross_ref[512:] = total[512 + rest :].astype(BF16)


def own_kernel(blocks, *refs):
    refs[-1][...] = caption_sum(refs, blocks, slice(0, 512))


def combine_kernel(down_a, down_b, over_head, up_a, up_b, over_tail, plus_ref, minus_ref):
    rows = down_a.shape[0]
    plus_ref[:rows] = (down_a[...] + over_head[...].astype(F32)).astype(BF16)
    plus_ref[rows:] = down_b[...]
    minus_ref[:rows] = up_a[...]
    minus_ref[rows:] = (up_b[...] + over_tail[...].astype(F32)).astype(BF16)


def back_kernel(own_ref, tail_ref, cross_ref, pair_ref, back_a, back_b):
    slots, rest = own_ref.shape[0], tail_ref.shape[0]
    pair = own_ref[...] + cross_ref[:slots].astype(F32)
    tail = tail_ref[...] + cross_ref[slots:].astype(F32)
    first = back_a.shape[0]
    pair_ref[...] = pair
    back_a[...] = pair[rest : rest + first].astype(BF16)
    back_b[: slots - rest - first] = pair[rest + first :].astype(BF16)
    back_b[slots - rest - first :] = tail.astype(BF16)


def image_kernel(raw_ref, own_ref, a_ref, b_ref, c_ref, far_ref, out_ref):
    count = own_ref.shape[0]
    sums = own_ref[...] + a_ref[:count].astype(F32) + b_ref[:count].astype(F32)
    sums = sums + c_ref[:count].astype(F32) + far_ref[...].astype(F32)
    out_ref[...] = project(raw_ref[...], sums)


def project(raw, sums):
    unit, inverse = unit_rows(raw)
    return (sums - unit * jnp.sum(unit * sums, axis=1, keepdims=True)) * inverse


def window_start(total, last, rows, slots):
    return pl.multiple_of(jnp.clip((total - last) // 16 * 16, 0, slots - rows), 16)


def home_kernel(
    last, total_ref, raw_ref, own_ref, back_ref, out_ref, part_raw, part_sums, sums_ref, grads_ref,
    sems,
):
    slots = own_ref.shape[0]
    rows = part_raw.shape[0]
    total = total_ref[0]
    steps = sems.shape[0]
    tile = slots // steps
    copies = []
    for step in range(steps):
        part = slice(step * tile, (step + 1) * tile)
        offset = slots - total + step * tile
        sums = own_ref[part] + picked(tile, back_ref.shape[0], offset, back_ref[...])
        sums_ref[part] = sums
        slot = step * tile + lax.broadcasted_iota(jnp.int32, sums.shape, 0)
        grads_ref[part] = jnp.where(slot < total, project(raw_ref[part], sums), 0.0)
        copies.append(
            pltpu.make_async_copy(grads_ref.at[part], out_ref.at[part], sems.at[step])
        )
        copies[-1].start()
    window = pl.ds(window_start(total, last, rows, slots), rows)
    part_raw[...] = raw_ref[window, :]
    part_sums[...] = sums_ref[window, :]
    for copy in copies:
        copy.wait()


def last_kernel(total_ref, raw_ref, sums_ref, back_ref, early_ref, out_ref, grads_ref, sem):
    last, rows = back_ref.shape[0], grads_ref.shape[0]
    total = total_ref[0]
    start = window_start(total, last, rows, out_ref.shape[0])
    sums = sums_ref[...] + picked(rows, last, start + last - total, back_ref[...])
    slot = start + lax.broadcasted_iota(jnp.int32, sums.shape, 0)
    grads_ref[...] = jnp.where(slot < total, project(raw_ref[...], sums), 0.0)
    copy = pltpu.make_async_copy(grads_ref, out_ref.at[pl.ds(start, rows), :], sem)
    copy.start()
    copy.wait()


def caption_grads(total, raw, own, back, last):
    slots, width = raw.shape
    rows = last + 16
    return pl.pallas_call(
        functools.partial(home_kernel, last),
        out_shape=(
            jax.ShapeDtypeStruct((slots, width), F32),
            jax.ShapeDtypeStruct((rows, width), BF16),
            jax.ShapeDtypeStruct((rows, width), F32),
        ),
        in_specs=[SMEM, VMEM, VMEM, VMEM],
        out_specs=(ANY, VMEM, VMEM),
        scratch_shapes=[
            pltpu.VMEM((slots, width), F32),
            pltpu.VMEM((slots, width), F32),
            pltpu.SemaphoreType.DMA((4,)),
        ],
        compiler_params=pltpu.CompilerParams(vmem_limit_bytes=20 * MIB),
        cost_estimate=pl.CostEstimate(
            flops=2 * slots * slots * width, bytes_accessed=8 * MIB, transcendentals=0
        ),
        name="caption_grad",
    )(total, raw, own, back)


def last_rows(total, raw, sums, back, early):
    slots, width = early.shape
    return pl.pallas_call(
        last_kernel,
        out_shape=jax.ShapeDtypeStruct((slots, width), F32),
        in_specs=[SMEM, VMEM, VMEM, VMEM, ANY],
        out_specs=ANY,
        scratch_shapes=[pltpu.VMEM(sums.shape, F32), pltpu.SemaphoreType.DMA],
        input_output_aliases={4: 0},
        compiler_params=pltpu.CompilerParams(vmem_limit_bytes=8 * MIB),
        cost_estimate=pl.CostEstimate(flops=10**6, bytes_accessed=MIB, transcendentals=0),
        name="caption_grad_last",
    )(total, raw, sums, back, early)


def program(image_embed, caption_vectors, caption_counts, natural_log_multiplier, match_odds_offset):
    count, width = image_embed.shape
    slots = caption_vectors.shape[0]
    pair_rows = 9 * count
    index = {a: lax.axis_index(a) for a in AXES}
    home = flat([index[a] for a in AXES])
    scale = jnp.exp(natural_log_multiplier[0])
    scalars = jnp.stack([scale, match_odds_offset[0]])

    partner_raw = send(caption_vectors, flip_route(0))
    far_raw = send(image_embed, flip_route(0, 4))

    counts = lax.dynamic_slice_in_dim(caption_counts, home * count, count)
    earlier = lax.iota(jnp.int32, count)[None, :] <= lax.iota(jnp.int32, count)[:, None]
    ends = jnp.sum(jnp.where(earlier, counts[None, :], 0), axis=1, keepdims=True)
    spans = jnp.concatenate([ends - counts[:, None], ends], axis=1)
    total = jnp.sum(counts).reshape(1)

    half = jax.ShapeDtypeStruct((4 * count, width), BF16)
    own_low = plain(low_kernel, jax.ShapeDtypeStruct((count, width), BF16), (image_embed,), limit=4)
    near = plain(
        near_kernel, jax.ShapeDtypeStruct((2 * count, width), BF16), (own_low, far_raw), limit=4
    )
    first = {}
    for k in (2, 1, 3):
        first[k] = send(near, ring_route(0, k))
    own_pad, pick = plain(
        prep_kernel,
        (
            jax.ShapeDtypeStruct((pair_rows, width), BF16),
            jax.ShapeDtypeStruct((pair_rows, slots), BF16),
        ),
        (total, caption_vectors),
        smem=1,
    )
    head, tail = plain(
        join_kernel, (half, half), (near, first[1], first[3], first[2]), after=(own_pad,)
    )
    up_head = send(head, ring_route(1, 1))
    down_tail = send(tail, ring_route(1, 3))
    up_tail = send(tail, ring_route(1, 1))
    down_head = send(head, ring_route(1, 3))
    two_head = send(up_head, ring_route(1, 1))
    two_tail = send(down_tail, ring_route(1, 3))

    own_pair = plain(
        merge_kernel,
        jax.ShapeDtypeStruct((pair_rows, width), BF16),
        (own_pad, pick, partner_raw),
        2 * pair_rows * slots * width,
        after=(head,),
    )
    other_pair = send(own_pair, flip_route(2))
    captions = plain(
        stack_kernel, jax.ShapeDtypeStruct((2 * pair_rows, width), BF16), (own_pair, other_pair)
    )

    def terms(head, tail, types, local=False, after=()):
        return weight_terms(local, types, scalars, spans, head, tail, captions, after)

    w_local, i_local = terms(head, tail, (), True)
    w_down, i_down, down_a, down_b = terms(down_head, down_tail, (F32, BF16), after=(w_local,))
    w_two, i_two, two_a, two_b = terms(two_head, two_tail, (BF16, BF16), after=(down_b,))
    over_head = send(two_a, ring_route(1, 1))
    over_tail = send(two_b, ring_route(1, 3))
    w_up, i_up, up_a, up_b = terms(up_head, up_tail, (BF16, F32), after=(two_a,))
    operands = [w_local, w_two, w_down, w_up, i_local, i_two, i_down, i_up]
    sum_flops = 2 * 32 * count * pair_rows * width
    cross, own_tail = plain(
        functools.partial(cross_kernel, 4),
        (
            jax.ShapeDtypeStruct((pair_rows, width), BF16),
            jax.ShapeDtypeStruct((pair_rows - slots, width), F32),
        ),
        operands,
        sum_flops,
        limit=24,
        after=(up_a,),
    )
    crossed = send(cross, flip_route(2))
    block_shape = jax.ShapeDtypeStruct((8 * count, width), BF16)
    plus, minus = plain(
        combine_kernel,
        (block_shape, block_shape),
        (down_a, down_b, over_head, up_a, up_b, over_tail),
        after=(cross,),
    )
    below = send(plus, ring_route(1, 1)).astype(F32)
    above = send(minus, ring_route(1, 3)).astype(F32)
    own_part = plain(
        functools.partial(own_kernel, 4),
        jax.ShapeDtypeStruct((slots, width), F32),
        operands,
        sum_flops,
        limit=24,
        after=(minus,),
    )
    last = 3 * slots // 8
    pair, back_a, back_b = plain(
        back_kernel,
        (
            jax.ShapeDtypeStruct((slots, width), F32),
            jax.ShapeDtypeStruct((slots - last, width), BF16),
            jax.ShapeDtypeStruct((last, width), BF16),
        ),
        (own_part, own_tail, crossed),
        limit=24,
    )
    returned_a = send(back_a, flip_route(0))
    returned_b = send(back_b, flip_route(0))
    half_sum = jax.ShapeDtypeStruct((4 * count, width), F32)
    local_a, local_b = plain(
        local_sums_kernel,
        (half_sum, half_sum),
        (w_local, captions),
        16 * count * 2 * pair_rows * width,
        after=(back_a,),
    )
    rows = 4 * count
    head_sum = local_a + below[:rows] + above[:rows]
    tail_sum = local_b + below[rows:] + above[rows:]

    near_rows = 2 * count
    pieces = {1: head_sum[near_rows:], 3: tail_sum[:near_rows], 2: tail_sum[near_rows:]}
    far_sum = head_sum[count:near_rows]
    near_back = []
    for k in (2, 1, 3):
        near_back.append(send(pieces[k].astype(BF16), ring_route(0, -k)))
        far_sum = far_sum + near_back[-1][count:].astype(F32)
    far_back = send(far_sum.astype(BF16), flip_route(0, 4))
    early_grad, part_raw, part_sums = caption_grads(total, caption_vectors, pair, returned_a, last)
    image_grad = plain(
        image_kernel,
        jax.ShapeDtypeStruct((count, width), F32),
        (image_embed, head_sum[:count], *near_back, far_back),
        limit=8,
    )
    caption_grad = last_rows(total, part_raw, part_sums, returned_b, early_grad)
    return image_grad, caption_grad


def solution(mesh):
    fine = Mesh(mesh.devices.reshape(SIZES), AXES)
    placed = (P(AXES, None), P(AXES, None), P(), P(), P())
    return jax.shard_map(
        program,
        mesh=fine,
        in_specs=placed,
        out_specs=(P(AXES, None), P(AXES, None)),
        check_vma=False,
    )
```

```python
import functools

import jax
import jax.numpy as jnp
from jax import lax
from jax.experimental import pallas as pl
from jax.experimental.pallas import tpu as pltpu
from jax.sharding import Mesh, PartitionSpec as P


EPSILON = 1e-06
LOG2E = 1.4426950408889634
AXES = ("y_lo", "x", "core", "z", "y_hi")
SIZES = (2, 4, 2, 4, 2)
F32 = jnp.float32
BF16 = jnp.bfloat16
VMEM = pl.BlockSpec(memory_space=pltpu.VMEM)
ANY = pl.BlockSpec(memory_space=pl.ANY)
SMEM = pl.BlockSpec(memory_space=pltpu.SMEM)
MIB = 2**20


def coordinates(device):
    out = []
    for size in reversed(SIZES):
        out.append(device % size)
        device //= size
    return out[::-1]


def flat(coords):
    device = 0
    for size, c in zip(SIZES, coords):
        device = device * size + c
    return device


def route(move):
    pairs = []
    for device in range(128):
        c = coordinates(device)
        move(c)
        pairs.append((device, flat(c)))
    return pairs


def ring_route(stage, distance):
    def move(c):
        axis = 1 if c[2] == stage else 3
        c[axis] = (c[axis] + distance) % 4

    return route(move)


def flip_route(*axes):
    def move(c):
        for axis in axes:
            c[axis] = 1 - c[axis]

    return route(move)


def send(value, pairs):
    return lax.ppermute(value, AXES, pairs)


def unit_rows(raw):
    values = raw.astype(F32)
    inverse = lax.rsqrt(jnp.sum(values * values, axis=1, keepdims=True) + EPSILON)
    return values * inverse, inverse


def low_kernel(raw_ref, out_ref):
    out_ref[...] = unit_rows(raw_ref[...])[0].astype(BF16)


def near_kernel(own_ref, far_ref, near_ref):
    count = own_ref.shape[0]
    near_ref[:count] = own_ref[...]
    near_ref[count:] = unit_rows(far_ref[...])[0].astype(BF16)


def join_kernel(a_ref, b_ref, c_ref, d_ref, head_ref, tail_ref, whole_ref):
    rows = a_ref.shape[0]
    for number, ref in enumerate((a_ref, b_ref, c_ref, d_ref)):
        half_ref = head_ref if number < 2 else tail_ref
        half_ref[number % 2 * rows : (number % 2 + 1) * rows] = ref[...]
        whole_ref[number * rows : (number + 1) * rows] = ref[...]


def plain(kernel, out_shape, args, flops=10**6, smem=0, limit=16, after=()):
    return pl.pallas_call(
        lambda *refs: kernel(*refs[: len(args)], *refs[len(args) + len(after) :]),
        out_shape=out_shape,
        in_specs=[SMEM] * smem + [VMEM] * (len(args) - smem) + [ANY] * len(after),
        out_specs=(VMEM,) * len(out_shape) if isinstance(out_shape, tuple) else VMEM,
        compiler_params=pltpu.CompilerParams(vmem_limit_bytes=limit * MIB),
        cost_estimate=pl.CostEstimate(flops=flops, bytes_accessed=MIB, transcendentals=0),
    )(*args, *after)


def prep_kernel(total_ref, own_ref, out_ref, pick_ref):
    slots = own_ref.shape[0]
    low = unit_rows(own_ref[...])[0]
    slot = lax.broadcasted_iota(jnp.int32, low.shape, 0)
    out_ref[:slots] = jnp.where(slot < total_ref[0], low, 0.0).astype(BF16)
    out_ref[slots:] = jnp.zeros((out_ref.shape[0] - slots, low.shape[1]), BF16)
    row = lax.broadcasted_iota(jnp.int32, pick_ref.shape, 0)
    column = lax.broadcasted_iota(jnp.int32, pick_ref.shape, 1)
    pick_ref[...] = jnp.where(column == row - total_ref[0], 1.0, 0.0).astype(BF16)


def picked(rows, columns, offset, values):
    row = lax.broadcasted_iota(jnp.int32, (rows, columns), 0)
    column = lax.broadcasted_iota(jnp.int32, (rows, columns), 1)
    pick = jnp.where(column == row + offset, 1.0, 0.0).astype(BF16)
    return jnp.dot(pick, values, preferred_element_type=F32)


def merge_kernel(own_ref, pick_ref, raw_ref, out_ref):
    low = unit_rows(raw_ref[...])[0].astype(BF16)
    other = jnp.dot(pick_ref[...], low, preferred_element_type=F32).astype(BF16)
    out_ref[...] = own_ref[...] + other


def stack_kernel(own_ref, other_ref, out_ref):
    rows = own_ref.shape[0]
    out_ref[:512] = own_ref[:512]
    out_ref[512:1024] = other_ref[:512]
    out_ref[1024 : rows + 512] = own_ref[512:]
    out_ref[rows + 512 :] = other_ref[512:]


def weigh(local, scalar_ref, spans_ref, images, captions, weight_ref):
    scale = scalar_ref[0]
    bias = scalar_ref[1]
    scores = lax.dot_general(
        images, captions, (((1,), (1,)), ((), ())), preferred_element_type=F32
    )
    steep = scores * (scale * -LOG2E) + (bias * -LOG2E)
    weight_ref[...] = (scale / (1.0 + jnp.exp2(steep))).astype(BF16)
    if local:
        count = spans_ref.shape[0]
        head = steep[:count, :512]
        slot = lax.broadcasted_iota(jnp.int32, head.shape, 1)
        match = (slot >= spans_ref[:, 0:1]) & (slot < spans_ref[:, 1:2])
        value = scale / (1.0 + jnp.exp2(jnp.where(match, -head, head)))
        weight_ref[:count, :512] = jnp.where(match, -value, value).astype(BF16)


def weight_kernel(
    local, sums, scalar_ref, spans_ref, head_ref, tail_ref, captions_ref, weight_ref, images_ref,
    *outs,
):
    rows = head_ref.shape[0]
    images_ref[:rows] = head_ref[...]
    images_ref[rows:] = tail_ref[...]
    weigh(local, scalar_ref, spans_ref, images_ref[...], captions_ref[...], weight_ref)
    if sums:
        total = jnp.dot(weight_ref[...], captions_ref[...], preferred_element_type=F32)
        outs[0][...] = total[:rows].astype(outs[0].dtype)
        outs[1][...] = total[rows:].astype(outs[1].dtype)


def weight_terms(local, types, scalars, spans, head, tail, captions, after=()):
    rows, width = head.shape
    slots = captions.shape[0]
    arity = 5
    return pl.pallas_call(
        lambda *refs: weight_kernel(
            local, bool(types), *refs[:arity], *refs[arity + len(after) :]
        ),
        out_shape=(
            jax.ShapeDtypeStruct((2 * rows, slots), BF16),
            jax.ShapeDtypeStruct((2 * rows, width), BF16),
            *[jax.ShapeDtypeStruct((rows, width), t) for t in types],
        ),
        in_specs=[SMEM] + [VMEM] * (arity - 1) + [ANY] * len(after),
        out_specs=(VMEM,) * (2 + len(types)),
        compiler_params=pltpu.CompilerParams(vmem_limit_bytes=20 * MIB),
        cost_estimate=pl.CostEstimate(
            flops=(8 if types else 4) * rows * slots * width,
            bytes_accessed=8 * MIB,
            transcendentals=2 * rows * slots,
        ),
        name="block_local" if local else "block_remote",
    )(scalars, spans, head, tail, captions, *after)


def local_kernel(scalar_ref, spans_ref, images_ref, captions_ref, weight_ref):
    weigh(True, scalar_ref, spans_ref, images_ref[...], captions_ref[...], weight_ref)


def local_sums_kernel(weight_ref, captions_ref, head_out, tail_out):
    rows = head_out.shape[0]
    total = jnp.dot(weight_ref[...], captions_ref[...], preferred_element_type=F32)
    head_out[...] = total[:rows]
    tail_out[...] = total[rows:]


def caption_sum(refs, blocks, columns):
    total = None
    for weight_ref, images_ref in zip(refs[:blocks], refs[blocks : 2 * blocks]):
        part = lax.dot_general(
            weight_ref[:, columns], images_ref[...], (((0,), (0,)), ((), ())),
            preferred_element_type=F32,
        )
        total = part if total is None else total + part
    return total


def cross_kernel(blocks, *refs):
    cross_ref, tail_ref = refs[-2:]
    rest = tail_ref.shape[0]
    total = caption_sum(refs, blocks, slice(512, refs[0].shape[1]))
    cross_ref[:512] = total[:512].astype(BF16)
    tail_ref[...] = total[512 : 512 + rest]
    cross_ref[512:] = total[512 + rest :].astype(BF16)


def own_kernel(blocks, *refs):
    refs[-1][...] = caption_sum(refs, blocks, slice(0, 512))


def combine_kernel(down_a, down_b, over_head, up_a, up_b, over_tail, plus_ref, minus_ref):
    rows = down_a.shape[0]
    plus_ref[:rows] = (down_a[...] + over_head[...].astype(F32)).astype(BF16)
    plus_ref[rows:] = down_b[...]
    minus_ref[:rows] = up_a[...]
    minus_ref[rows:] = (up_b[...] + over_tail[...].astype(F32)).astype(BF16)


def back_kernel(own_ref, tail_ref, cross_ref, pair_ref, back_a, back_b):
    slots, rest = own_ref.shape[0], tail_ref.shape[0]
    pair = own_ref[...] + cross_ref[:slots].astype(F32)
    tail = tail_ref[...] + cross_ref[slots:].astype(F32)
    first = back_a.shape[0]
    pair_ref[...] = pair
    back_a[...] = pair[rest : rest + first].astype(BF16)
    back_b[: slots - rest - first] = pair[rest + first :].astype(BF16)
    back_b[slots - rest - first :] = tail.astype(BF16)


def image_kernel(raw_ref, own_ref, a_ref, b_ref, c_ref, far_ref, out_ref):
    count = own_ref.shape[0]
    sums = own_ref[...] + a_ref[:count].astype(F32) + b_ref[:count].astype(F32)
    sums = sums + c_ref[:count].astype(F32) + far_ref[...].astype(F32)
    out_ref[...] = project(raw_ref[...], sums)


def project(raw, sums):
    unit, inverse = unit_rows(raw)
    return (sums - unit * jnp.sum(unit * sums, axis=1, keepdims=True)) * inverse


def window_start(total, last, rows, slots):
    return pl.multiple_of(jnp.clip((total - last) // 16 * 16, 0, slots - rows), 16)


def home_kernel(
    last, total_ref, raw_ref, own_ref, back_ref, out_ref, part_raw, part_sums, sums_ref, grads_ref,
    sems,
):
    slots = own_ref.shape[0]
    rows = part_raw.shape[0]
    total = total_ref[0]
    steps = sems.shape[0]
    tile = slots // steps
    copies = []
    for step in range(steps):
        part = slice(step * tile, (step + 1) * tile)
        offset = slots - total + step * tile
        sums = own_ref[part] + picked(tile, back_ref.shape[0], offset, back_ref[...])
        sums_ref[part] = sums
        slot = step * tile + lax.broadcasted_iota(jnp.int32, sums.shape, 0)
        grads_ref[part] = jnp.where(slot < total, project(raw_ref[part], sums), 0.0)
        copies.append(
            pltpu.make_async_copy(grads_ref.at[part], out_ref.at[part], sems.at[step])
        )
        copies[-1].start()
    window = pl.ds(window_start(total, last, rows, slots), rows)
    part_raw[...] = raw_ref[window, :]
    part_sums[...] = sums_ref[window, :]
    for copy in copies:
        copy.wait()


def last_kernel(total_ref, raw_ref, sums_ref, back_ref, early_ref, out_ref, grads_ref, sem):
    last, rows = back_ref.shape[0], grads_ref.shape[0]
    total = total_ref[0]
    start = window_start(total, last, rows, out_ref.shape[0])
    sums = sums_ref[...] + picked(rows, last, start + last - total, back_ref[...])
    slot = start + lax.broadcasted_iota(jnp.int32, sums.shape, 0)
    grads_ref[...] = jnp.where(slot < total, project(raw_ref[...], sums), 0.0)
    copy = pltpu.make_async_copy(grads_ref, out_ref.at[pl.ds(start, rows), :], sem)
    copy.start()
    copy.wait()


def caption_grads(total, raw, own, back, last):
    slots, width = raw.shape
    rows = last + 16
    return pl.pallas_call(
        functools.partial(home_kernel, last),
        out_shape=(
            jax.ShapeDtypeStruct((slots, width), F32),
            jax.ShapeDtypeStruct((rows, width), BF16),
            jax.ShapeDtypeStruct((rows, width), F32),
        ),
        in_specs=[SMEM, VMEM, VMEM, VMEM],
        out_specs=(ANY, VMEM, VMEM),
        scratch_shapes=[
            pltpu.VMEM((slots, width), F32),
            pltpu.VMEM((slots, width), F32),
            pltpu.SemaphoreType.DMA((4,)),
        ],
        compiler_params=pltpu.CompilerParams(vmem_limit_bytes=20 * MIB),
        cost_estimate=pl.CostEstimate(
            flops=2 * slots * slots * width, bytes_accessed=8 * MIB, transcendentals=0
        ),
        name="caption_grad",
    )(total, raw, own, back)


def last_rows(total, raw, sums, back, early):
    slots, width = early.shape
    return pl.pallas_call(
        last_kernel,
        out_shape=jax.ShapeDtypeStruct((slots, width), F32),
        in_specs=[SMEM, VMEM, VMEM, VMEM, ANY],
        out_specs=ANY,
        scratch_shapes=[pltpu.VMEM(sums.shape, F32), pltpu.SemaphoreType.DMA],
        input_output_aliases={4: 0},
        compiler_params=pltpu.CompilerParams(vmem_limit_bytes=8 * MIB),
        cost_estimate=pl.CostEstimate(flops=10**6, bytes_accessed=MIB, transcendentals=0),
        name="caption_grad_last",
    )(total, raw, sums, back, early)


def program(image_embed, caption_vectors, caption_counts, natural_log_multiplier, match_odds_offset):
    count, width = image_embed.shape
    slots = caption_vectors.shape[0]
    pair_rows = 9 * count
    index = {a: lax.axis_index(a) for a in AXES}
    home = flat([index[a] for a in AXES])
    scale = jnp.exp(natural_log_multiplier[0])
    scalars = jnp.stack([scale, match_odds_offset[0]])

    partner_raw = send(caption_vectors, flip_route(0))
    far_raw = send(image_embed, flip_route(0, 4))

    counts = lax.dynamic_slice_in_dim(caption_counts, home * count, count)
    earlier = lax.iota(jnp.int32, count)[None, :] <= lax.iota(jnp.int32, count)[:, None]
    ends = jnp.sum(jnp.where(earlier, counts[None, :], 0), axis=1, keepdims=True)
    spans = jnp.concatenate([ends - counts[:, None], ends], axis=1)
    total = jnp.sum(counts).reshape(1)

    half = jax.ShapeDtypeStruct((4 * count, width), BF16)
    own_low = plain(low_kernel, jax.ShapeDtypeStruct((count, width), BF16), (image_embed,), limit=4)
    near = plain(
        near_kernel, jax.ShapeDtypeStruct((2 * count, width), BF16), (own_low, far_raw), limit=4
    )
    first = {}
    for k in (2, 1, 3):
        first[k] = send(near, ring_route(0, k))
    own_pad, pick = plain(
        prep_kernel,
        (
            jax.ShapeDtypeStruct((pair_rows, width), BF16),
            jax.ShapeDtypeStruct((pair_rows, slots), BF16),
        ),
        (total, caption_vectors),
        smem=1,
    )
    head, tail, i_local = plain(
        join_kernel,
        (half, half, jax.ShapeDtypeStruct((8 * count, width), BF16)),
        (near, first[1], first[3], first[2]),
        after=(own_pad,),
    )
    up_head = send(head, ring_route(1, 1))
    down_tail = send(tail, ring_route(1, 3))
    up_tail = send(tail, ring_route(1, 1))
    down_head = send(head, ring_route(1, 3))
    two_head = send(up_head, ring_route(1, 1))
    two_tail = send(down_tail, ring_route(1, 3))

    own_pair = plain(
        merge_kernel,
        jax.ShapeDtypeStruct((pair_rows, width), BF16),
        (own_pad, pick, partner_raw),
        2 * pair_rows * slots * width,
        after=(head,),
    )
    other_pair = send(own_pair, flip_route(2))
    captions = plain(
        stack_kernel, jax.ShapeDtypeStruct((2 * pair_rows, width), BF16), (own_pair, other_pair)
    )

    def terms(head, tail, types, local=False, after=()):
        return weight_terms(local, types, scalars, spans, head, tail, captions, after)

    w_local = plain(
        local_kernel,
        jax.ShapeDtypeStruct((8 * count, 2 * pair_rows), BF16),
        (scalars, spans, i_local, captions),
        32 * count * pair_rows * width,
        1,
        20,
    )
    w_down, i_down, down_a, down_b = terms(down_head, down_tail, (F32, BF16), after=(w_local,))
    w_two, i_two, two_a, two_b = terms(two_head, two_tail, (BF16, BF16), after=(down_b,))
    over_head = send(two_a, ring_route(1, 1))
    over_tail = send(two_b, ring_route(1, 3))
    w_up, i_up, up_a, up_b = terms(up_head, up_tail, (BF16, F32), after=(two_a,))
    operands = [w_local, w_two, w_down, w_up, i_local, i_two, i_down, i_up]
    sum_flops = 2 * 32 * count * pair_rows * width
    cross, own_tail = plain(
        functools.partial(cross_kernel, 4),
        (
            jax.ShapeDtypeStruct((pair_rows, width), BF16),
            jax.ShapeDtypeStruct((pair_rows - slots, width), F32),
        ),
        operands,
        sum_flops,
        limit=24,
        after=(up_a,),
    )
    crossed = send(cross, flip_route(2))
    block_shape = jax.ShapeDtypeStruct((8 * count, width), BF16)
    plus, minus = plain(
        combine_kernel,
        (block_shape, block_shape),
        (down_a, down_b, over_head, up_a, up_b, over_tail),
        after=(cross,),
    )
    below = send(plus, ring_route(1, 1)).astype(F32)
    above = send(minus, ring_route(1, 3)).astype(F32)
    own_part = plain(
        functools.partial(own_kernel, 4),
        jax.ShapeDtypeStruct((slots, width), F32),
        operands,
        sum_flops,
        limit=24,
        after=(minus,),
    )
    last = 3 * slots // 8
    pair, back_a, back_b = plain(
        back_kernel,
        (
            jax.ShapeDtypeStruct((slots, width), F32),
            jax.ShapeDtypeStruct((slots - last, width), BF16),
            jax.ShapeDtypeStruct((last, width), BF16),
        ),
        (own_part, own_tail, crossed),
        limit=24,
    )
    returned_a = send(back_a, flip_route(0))
    returned_b = send(back_b, flip_route(0))
    half_sum = jax.ShapeDtypeStruct((4 * count, width), F32)
    local_a, local_b = plain(
        local_sums_kernel,
        (half_sum, half_sum),
        (w_local, captions),
        16 * count * 2 * pair_rows * width,
        after=(back_a,),
    )
    rows = 4 * count
    head_sum = local_a + below[:rows] + above[:rows]
    tail_sum = local_b + below[rows:] + above[rows:]

    near_rows = 2 * count
    pieces = {1: head_sum[near_rows:], 3: tail_sum[:near_rows], 2: tail_sum[near_rows:]}
    far_sum = head_sum[count:near_rows]
    near_back = []
    for k in (2, 1, 3):
        near_back.append(send(pieces[k].astype(BF16), ring_route(0, -k)))
        far_sum = far_sum + near_back[-1][count:].astype(F32)
    far_back = send(far_sum.astype(BF16), flip_route(0, 4))
    early_grad, part_raw, part_sums = caption_grads(total, caption_vectors, pair, returned_a, last)
    image_grad = plain(
        image_kernel,
        jax.ShapeDtypeStruct((count, width), F32),
        (image_embed, head_sum[:count], *near_back, far_back),
        limit=8,
    )
    caption_grad = last_rows(total, part_raw, part_sums, returned_b, early_grad)
    return image_grad, caption_grad


def solution(mesh):
    fine = Mesh(mesh.devices.reshape(SIZES), AXES)
    placed = (P(AXES, None), P(AXES, None), P(), P(), P())
    return jax.shard_map(
        program,
        mesh=fine,
        in_specs=placed,
        out_specs=(P(AXES, None), P(AXES, None)),
        check_vma=False,
    )
```
